512 devices in a mesh: nodes: 128 (over z, x, core), mp: 4 (over y).
Axes of the slice: x: 4, y: 4, z: 16, core: 2. Of those that a mesh axis runs over, the one named last changes fastest.
Arguments:
- grid_in: bfloat16 [131072, 1024], P('nodes', 'mp'), may hold values from -2200 to 2200
- mesh_in: bfloat16 [32768, 1024], P('nodes', 'mp'), may hold values from -2200 to 2200
- w_query: bfloat16 [4, 1024, 512], P(None, None, 'mp'), as said below
- w_key: bfloat16 [4, 1024, 512], P(None, None, 'mp'), may hold values from -8 to 8
- w_value: bfloat16 [4, 1024, 512], P(None, None, 'mp'), may hold values from -0.1875 to 0.1875
- w_out: bfloat16 [4, 512, 1024], P(None, 'mp'), may hold values from -1 to 1
- norm_gains: float32 [6, 1024], replicated, may hold values from 0.25 to 1.75
- enc_list: int32 [256, 4], P('nodes'), may hold values from 0 to 1023, as said below
- proc_list: int32 [256, 3], P('nodes'), may hold values from 0 to 255, as said below
- dec_list: int32 [1024, 2], P('nodes'), may hold values from 0 to 255, as said below
- grid_count: int32 [1024], replicated, may hold values from 1 to 128
Outputs:
- grid_out: bfloat16 [131072, 1024], P('nodes', 'mp')
- mesh_out: bfloat16 [32768, 1024], P('nodes', 'mp')
The draws below stay inside these ranges and needn't reach their ends.
Inputs may be any that keep to these rules, and one draw needn't show every extreme that they name: `enc_list`: mesh block b lies with node index b // 2; its 4 entries are distinct grid blocks held by node indices at most 2 from it (grid block c lies with node index c // 8). `proc_list`: entry 0 of row b is b; the others are distinct mesh blocks other than b held by node indices at most 2 from b's. `dec_list`: grid block c's 2 entries are distinct mesh blocks held by node indices at most 2 from c's. `w_query`: entries within 6 / sqrt(1024) of zero.
All inputs are finite; a program needn't handle non-finite values.
Results may differ from the reference program's by a relative error of at most 0.019.
Values may be sent and summed in bfloat16 or wider, within the bound.
No kernel may reach another device: no remote copies, remote signals or barrier semaphores. Data moves between devices by JAX's collectives and lax.ppermute only.
A program may use at most 64 MiB of HBM per device.

```python
import jax
import jax.numpy as jnp
from jax import lax

D = 1024
HEADS = 8
HEAD_DIM = 64
BLOCK = 128
REACH = 2
LIST_ENC = 4
LIST_PROC = 3
LIST_DEC = 2
GB_DEV = 8
MB_DEV = 2
HD = 512
GRID_BLOCKS = 1024
MESH_BLOCKS = 256
N_MP = 4


def drawn_rows(key, row_count, salt):
    return jnp.clip(jax.random.normal(jax.random.fold_in(key, salt), (row_count, D)), -6.0, 6.0)


def draw_grid_in(key, part):
    states = drawn_rows(key, GRID_BLOCKS * BLOCK, 11)
    return states.astype(jnp.bfloat16)


def draw_mesh_in(key, part):
    states = drawn_rows(key, MESH_BLOCKS * BLOCK, 21)
    return states.astype(jnp.bfloat16)


def query_table(key):
    return jnp.clip(jax.random.normal(jax.random.fold_in(key, 31), (4, D, HEADS * HEAD_DIM)), -6.0, 6.0) * D ** (-0.5)


def draw_w_query(key, part):
    return query_table(key).astype(jnp.bfloat16)


def draw_w_key(key, part):
    noise = jnp.clip(jax.random.normal(jax.random.fold_in(key, 41), (4, D, HEADS * HEAD_DIM)), -6.0, 6.0) * D ** (-0.5)
    result = noise
    return result.astype(jnp.bfloat16)


def pick_window(key, query_blocks, per_query, per_key, key_total, count, skip_self):
    width_blocks = (2 * REACH + 1) * per_key
    device_of = jnp.arange(query_blocks) // per_query
    window_start = (device_of - REACH) * per_key
    positions = jnp.arange(width_blocks)
    candidate = window_start[:, None] + positions[None, :]
    usable = (candidate >= 0) & (candidate < key_total)
    if skip_self:
        usable = usable & (candidate != jnp.arange(query_blocks)[:, None])
    priority = jax.random.randint(key, (query_blocks, width_blocks), 0, 1 << 20) * width_blocks + positions[None, :]
    priority = jnp.where(usable, priority, -1 - positions[None, :])
    highest, places = lax.top_k(priority, count)
    return (window_start[:, None] + places).astype(jnp.int32)


def draw_enc_list(key, part):
    return pick_window(jax.random.fold_in(key, 51), MESH_BLOCKS, MB_DEV, GB_DEV, GRID_BLOCKS, LIST_ENC, False)


def draw_proc_list(key, part):
    others = pick_window(jax.random.fold_in(key, 52), MESH_BLOCKS, MB_DEV, MB_DEV, MESH_BLOCKS, LIST_PROC - 1, True)
    itself = jnp.arange(MESH_BLOCKS).astype(jnp.int32)[:, None]
    return jnp.concatenate([itself, others], axis=1).astype(jnp.int32)


def draw_dec_list(key, part):
    return pick_window(jax.random.fold_in(key, 53), GRID_BLOCKS, GB_DEV, MB_DEV, MESH_BLOCKS, LIST_DEC, False)


def with_ends(values, own_key, least, top_value):
    extent = values.shape
    place = [jax.random.randint(jax.random.fold_in(own_key, axis), (), 0, extent[axis]) for axis in range(len(extent))]
    values = values.at[tuple(place)].set(least)
    longest = extent.index(max(extent))
    place[longest] = (place[longest] + 1) % extent[longest]
    return values.at[tuple(place)].set(top_value)


def steps_of(own_key, extent, shards, smallest, high):
    def one(position, blocks):
        heights = jax.random.uniform(jax.random.fold_in(jax.random.fold_in(own_key, 6), position), (blocks,), jnp.float32, smallest / len(shards), high / len(shards))
        return jnp.repeat(jnp.exp(heights), extent[position] // blocks).reshape((-1,) + (1,) * (len(extent) - position - 1))

    factor_of = one(*shards[0])
    for cut in shards[1:]:
        factor_of = factor_of * one(*cut)
    return factor_of


def normal_values(own_key, extent, scale, bound, split=(), held_as=jnp.bfloat16):
    drawn = scale * jax.random.normal(own_key, extent, jnp.float32)
    if split:
        drawn = drawn * steps_of(own_key, extent, split, -0.22, 0.18)
    return jnp.clip(drawn, -bound, bound).astype(held_as)


def setup_inputs(seed: int = 0) -> dict:
    arg_keys = jax.random.split(jax.random.key(seed), 12)
    return {
        "grid_in": draw_grid_in(jax.random.fold_in(arg_keys[11], 71), 0),
        "mesh_in": draw_mesh_in(jax.random.fold_in(arg_keys[11], 71), 0),
        "w_query": draw_w_query(jax.random.fold_in(arg_keys[11], 71), 0),
        "w_key": draw_w_key(jax.random.fold_in(arg_keys[11], 71), 0),
        "w_value": normal_values(arg_keys[4], (4, D, HD), D ** -0.5, 0.1875, ((2, 4),)),
        "w_out": normal_values(arg_keys[5], (4, HD, D), (HD // 16) ** -0.5, 1.0, ((1, 4),)),
        "norm_gains": jnp.clip(1.0 + 0.15 * jax.random.normal(arg_keys[6], (6, D), jnp.float32), 0.25, 1.75),
        "enc_list": draw_enc_list(jax.random.fold_in(arg_keys[11], 71), 0),
        "proc_list": draw_proc_list(jax.random.fold_in(arg_keys[11], 71), 0),
        "dec_list": draw_dec_list(jax.random.fold_in(arg_keys[11], 71), 0),
        "grid_count": with_ends(jax.random.randint(arg_keys[10], (GRID_BLOCKS,), 1, BLOCK + 1), jax.random.fold_in(arg_keys[10], 1), 1, BLOCK).astype(jnp.int32),
    }


epsilon = 1e-05

def normalize(states, gains):
    values = states.astype(jnp.float32)
    average = lax.optimization_barrier(jnp.mean(values, axis=-1, keepdims=True))
    centred = values - average
    spread = lax.optimization_barrier(jnp.mean(centred * centred, axis=-1, keepdims=True))
    return (centred * lax.rsqrt(spread + epsilon) * gains).astype(jnp.bfloat16)

def project(inputs, weight):
    return jnp.dot(inputs, weight, preferred_element_type=jnp.float32).astype(jnp.bfloat16)

def attend(queries, key_rows, values, key_ok):
    batch_count, row_count, head_width = queries.shape
    key_count = key_rows.shape[1]
    head_count = head_width // HEAD_DIM
    query_heads = queries.reshape(batch_count, row_count, head_count, HEAD_DIM).astype(jnp.float32)
    key_heads = key_rows.reshape(batch_count, key_count, head_count, HEAD_DIM).astype(jnp.float32)
    value_heads = values.reshape(batch_count, key_count, head_count, HEAD_DIM).astype(jnp.float32)
    scores = jnp.einsum('brhd,bkhd->bhrk', query_heads, key_heads) * HEAD_DIM ** (-0.5)
    if key_ok is not None:
        scores = jnp.where(key_ok[:, None, None, :], scores, -1e+30)
    highest = lax.optimization_barrier(jnp.max(scores, axis=-1, keepdims=True))
    weights = jnp.exp(scores - highest)
    chances = (weights / lax.optimization_barrier(jnp.sum(weights, axis=-1, keepdims=True))).astype(jnp.bfloat16)
    blended = jnp.einsum('bhrk,bkhd->brhd', chances.astype(jnp.float32), value_heads)
    return blended.astype(jnp.bfloat16).reshape(batch_count * row_count, head_width)

def out_projection(blended, weight):
    group_width = weight.shape[0] // N_MP
    summed = jnp.zeros((blended.shape[0], weight.shape[1]), jnp.float32)
    for member in range(N_MP):
        piece = jnp.dot(blended[:, member * group_width:(member + 1) * group_width], weight[member * group_width:(member + 1) * group_width], preferred_element_type=jnp.float32).astype(jnp.bfloat16)
        piece = lax.optimization_barrier(piece)
        summed = summed + piece.astype(jnp.float32)
    return summed

def gather_blocks(source, listed):
    chosen = source[listed]
    return chosen.reshape(listed.shape[0], listed.shape[1] * BLOCK, source.shape[2])

def reference(grid_in, mesh_in, w_query, w_key, w_value, w_out, norm_gains, enc_list, proc_list, dec_list, grid_count):
    head_width = w_query.shape[2]
    row_ok = jnp.arange(BLOCK)[None, :] < grid_count[:, None]
    mesh_queries = project(normalize(mesh_in, norm_gains[0]), w_query[0]).reshape(-1, BLOCK, head_width)
    grid_normed = normalize(grid_in, norm_gains[1])
    grid_keys = project(grid_normed, w_key[0]).reshape(-1, BLOCK, head_width)
    grid_values = project(grid_normed, w_value[0]).reshape(-1, BLOCK, head_width)
    listed_ok = row_ok[enc_list].reshape(enc_list.shape[0], -1)
    blended = attend(mesh_queries, gather_blocks(grid_keys, enc_list), gather_blocks(grid_values, enc_list), listed_ok)
    mesh = (mesh_in.astype(jnp.float32) + out_projection(blended, w_out[0])).astype(jnp.bfloat16)
    for layer_index in (1, 2):
        normed = normalize(mesh, norm_gains[layer_index + 1])
        queries = project(normed, w_query[layer_index]).reshape(-1, BLOCK, head_width)
        mesh_keys = project(normed, w_key[layer_index]).reshape(-1, BLOCK, head_width)
        mesh_values = project(normed, w_value[layer_index]).reshape(-1, BLOCK, head_width)
        blended = attend(queries, gather_blocks(mesh_keys, proc_list), gather_blocks(mesh_values, proc_list), None)
        mesh = (mesh.astype(jnp.float32) + out_projection(blended, w_out[layer_index])).astype(jnp.bfloat16)
    grid_queries = project(normalize(grid_in, norm_gains[4]), w_query[3]).reshape(-1, BLOCK, head_width)
    mesh_normed = normalize(mesh, norm_gains[5])
    mesh_keys = project(mesh_normed, w_key[3]).reshape(-1, BLOCK, head_width)
    mesh_values = project(mesh_normed, w_value[3]).reshape(-1, BLOCK, head_width)
    blended = attend(grid_queries, gather_blocks(mesh_keys, dec_list), gather_blocks(mesh_values, dec_list), None)
    grid_out = grid_in.astype(jnp.float32) + out_projection(blended, w_out[3])
    grid_out = jnp.where(row_ok.reshape(-1, 1), grid_out, 0.0).astype(jnp.bfloat16)
    return (grid_out, mesh)
```

```python
import jax
import jax.numpy as jnp
from jax import lax
from jax.experimental import pallas as pl
from jax.experimental.pallas import tpu as pltpu
from jax.sharding import PartitionSpec as P


BLOCK = 128
REACH = 2
EPS = 1e-05
MP = 4
F32 = jnp.float32
BF16 = jnp.bfloat16

ENC0, PROC0, DEC0 = 2, 10, 16


PARAMS = pltpu.CompilerParams(vmem_limit_bytes=16 * 1024 * 1024)


def shift_mp(value, steps):
    return lax.ppermute(value, "mp", [(s, (s + steps) % MP) for s in range(MP)])


def from_node(value, offset):
    count = lax.axis_size("nodes")
    pairs = [(s, s - offset) for s in range(count) if 0 <= s - offset < count]
    return lax.ppermute(value, "nodes", pairs)


def swap_cores(value):
    count = lax.axis_size("nodes")
    return lax.ppermute(value, "nodes", [(s, s ^ 1) for s in range(count)])


def smem():
    return pl.BlockSpec(memory_space=pltpu.SMEM)


def vmem():
    return pl.BlockSpec(memory_space=pltpu.VMEM)


def source(meta, k):
    return (meta[0] + MP - k) % MP


def normed(pieces):
    width = sum(p.shape[-1] for p in pieces)
    values = [p.astype(F32) for p in pieces]
    mean = sum(jnp.sum(v, axis=-1, keepdims=True) for v in values) * (1.0 / width)
    centred = [v - mean for v in values]
    spread = sum(jnp.sum(c * c, axis=-1, keepdims=True) for c in centred) * (1.0 / width)
    scale = lax.rsqrt(spread + EPS)
    return [c * scale for c in centred]


def dot(a, b):
    return jnp.dot(a, b, preferred_element_type=F32)


def grid_kernel(meta, x0, x1, x2, x3, gains, w_k, w_v, w_q, kv_out, q_out):
    rows = normed([x[...] for x in (x0, x1, x2, x3)])
    kv = q = None
    for k in range(MP):
        src = source(meta, k)
        at = pl.ds(pl.multiple_of(src * 256, 256), 256)
        for_kv = (rows[k] * gains[1, pl.ds(src, 1), :]).astype(BF16)
        for_q = (rows[k] * gains[4, pl.ds(src, 1), :]).astype(BF16)
        kv_part = dot(for_kv, jnp.concatenate([w_k[at, :], w_v[at, :]], axis=1))
        q_part = dot(for_q, w_q[at, :])
        kv = kv_part if kv is None else kv + kv_part
        q = q_part if q is None else q + q_part
    kv_out[...] = kv.astype(BF16)
    q_out[...] = q.astype(BF16)


def grid_project(meta, pieces, gains, w_k, w_v, w_q):
    rows = pieces[0].shape[0]
    tile = 256
    return pl.pallas_call(
        grid_kernel,
        grid=(rows // tile,),
        in_specs=[smem()]
        + [pl.BlockSpec((tile, 256), lambda i: (i, 0))] * MP
        + [vmem()] * 4,
        out_specs=[
            pl.BlockSpec((tile, 256), lambda i: (i, 0)),
            pl.BlockSpec((tile, 128), lambda i: (i, 0)),
        ],
        out_shape=[
            jax.ShapeDtypeStruct((rows, 256), BF16),
            jax.ShapeDtypeStruct((rows, 128), BF16),
        ],
        cost_estimate=pl.CostEstimate(flops=rows * 1024 * 384 * 2, transcendentals=0, bytes_accessed=rows * 4096),
        compiler_params=PARAMS,
        name="grid_project",
    )(meta, *pieces, gains, w_k, w_v, w_q)


def mesh_kernel(meta, x0, x1, x2, x3, gains, w_q, state_out, q_out):
    pieces = [x[...] for x in (x0, x1, x2, x3)]
    rows = normed(pieces)
    q = None
    for k in range(MP):
        src = source(meta, k)
        at = pl.ds(pl.multiple_of(src * 256, 256), 256)
        part = dot((rows[k] * gains[0, pl.ds(src, 1), :]).astype(BF16), w_q[at, :])
        q = part if q is None else q + part
        state_out[src] = pieces[k]
    q_out[...] = q.astype(BF16)


def mesh_start(meta, pieces, gains, w_q):
    rows = pieces[0].shape[0]
    return pl.pallas_call(
        mesh_kernel,
        in_specs=[smem()] + [vmem()] * 6,
        out_specs=[vmem(), vmem()],
        out_shape=[
            jax.ShapeDtypeStruct((MP, rows, 256), BF16),
            jax.ShapeDtypeStruct((rows, 128), BF16),
        ],
        cost_estimate=pl.CostEstimate(flops=rows * 1024 * 128 * 2, transcendentals=0, bytes_accessed=rows * 4096),
        compiler_params=PARAMS,
        name="mesh_start",
    )(meta, *pieces, gains, w_q)


def head_rows():
    lane = lax.broadcasted_iota(jnp.int32, (1, 128), 1)
    first = jnp.where(lane < 64, 0.125, 0.0).astype(BF16)
    second = jnp.where(lane < 64, 0.0, 0.125).astype(BF16)
    return first, second


def attend_block(q, keys, values, key_ok):
    outs = []
    for row in head_rows():
        scores = lax.dot_general(
            q * row, keys, (((1,), (1,)), ((), ())), preferred_element_type=F32
        )
        if key_ok is not None:
            scores = jnp.where(key_ok, scores, -1e30)
        highest = jnp.max(scores, axis=-1, keepdims=True)
        weights = jnp.exp(scores - highest)
        total = jnp.sum(weights, axis=-1, keepdims=True)
        outs.append(dot(weights.astype(BF16), values) / total)
    lane = lax.broadcasted_iota(jnp.int32, outs[0].shape, 1)
    return jnp.where(lane < 64, outs[0], outs[1]).astype(BF16)


def enc_kernel(meta, listed, counts, q, *rest):
    windows, o_out, kept = rest[:-2], rest[-2], rest[-1]
    blocks_each = windows[0].shape[0] // BLOCK
    for slot in range(8):
        place = meta[ENC0 + slot]
        which = place // blocks_each
        start = pl.multiple_of((place % blocks_each) * BLOCK, BLOCK)
        for i, array in enumerate(windows):

            @pl.when(which == i)
            def _():
                kept[slot] = array[pl.ds(start, BLOCK), :]

    lane = lax.broadcasted_iota(jnp.int32, (1, BLOCK), 1)
    for b in range(2):
        key_ok = jnp.concatenate(
            [lane < counts[listed[b, j]] for j in range(4)], axis=1
        )
        kv = kept[b * 4 : b * 4 + 4].reshape(4 * BLOCK, 256)
        o = attend_block(q[b * BLOCK : (b + 1) * BLOCK, :], kv[:, :128], kv[:, 128:], key_ok)
        for j in range(MP):
            o_out[j, b * BLOCK : (b + 1) * BLOCK, :] = o


def enc_attend(meta, listed, counts, q, windows):
    return pl.pallas_call(
        enc_kernel,
        in_specs=[smem(), smem(), smem()] + [vmem()] * (1 + len(windows)),
        out_specs=vmem(),
        out_shape=jax.ShapeDtypeStruct((MP,) + q.shape, BF16),
        scratch_shapes=[pltpu.VMEM((8, BLOCK, 256), BF16)],
        compiler_params=PARAMS,
        name="enc_attend",
    )(meta, listed, counts, q, *windows)


def near_kernel(first_entry, per_block, meta, q, a0, a1, a2, a3, a4, o_out, kept):
    for i, array in enumerate((a0, a1, a2, a3, a4)):
        kept[2 * i] = array[0:BLOCK, :]
        kept[2 * i + 1] = array[BLOCK : 2 * BLOCK, :]
    for b in range(q.shape[0] // BLOCK):
        kv = jnp.concatenate(
            [kept[meta[first_entry + b * per_block + j]] for j in range(per_block)], axis=0
        )
        o = attend_block(q[b * BLOCK : (b + 1) * BLOCK, :], kv[:, :128], kv[:, 128:], None)
        for j in range(MP):
            o_out[j, b * BLOCK : (b + 1) * BLOCK, :] = o


def near_attend(first_entry, per_block, meta, q, windows):
    def body(*refs):
        near_kernel(first_entry, per_block, *refs)

    return pl.pallas_call(
        body,
        in_specs=[smem()] + [vmem()] * 6,
        out_specs=vmem(),
        out_shape=jax.ShapeDtypeStruct((MP,) + q.shape, BF16),
        scratch_shapes=[pltpu.VMEM((10, BLOCK, 256), BF16)],
        compiler_params=PARAMS,
        name="near_attend",
    )(meta, q, *windows)


def layer_kernel(index, gain_row, with_query, meta, o, state, w_own, a1, a2, a3, other, gains, *rest):
    projections, outs = rest[: 2 + with_query], rest[2 + with_query :]
    heads = jnp.concatenate([o[source(meta, k)] for k in range(MP)], axis=1)
    core = meta[1] % 2
    for part in range(4):
        at = 2 * index + part % 2
        if part < 2:
            g = 2 * core + part
            fetched = [a1[at], a2[at], a3[at]]
        else:
            g = 2 * (1 - core) + part - 2
            fetched = [other[k, at] for k in range(MP - 1)]
        w_out = jnp.concatenate([w_own[index, g]] + fetched, axis=0)
        outs[0][g] = (state[g].astype(F32) + dot(heads, w_out)).astype(BF16)
    rows = normed([outs[0][g] for g in range(MP)])
    row = jnp.concatenate(
        [(rows[g] * gains[gain_row, g : g + 1, :]).astype(BF16) for g in range(MP)], axis=1
    )
    result = dot(row, jnp.concatenate([w[...] for w in projections], axis=1)).astype(BF16)
    outs[1][...] = result[:, :256]
    if with_query:
        outs[2][...] = result[:, 256:]


def layer(index, gain_row, with_query, meta, o, state, w_own, fetched, other, gains, projections):
    def body(*refs):
        layer_kernel(index, gain_row, with_query, *refs)

    rows = state.shape[1]
    shapes = [
        jax.ShapeDtypeStruct(state.shape, BF16),
        jax.ShapeDtypeStruct((rows, 256), BF16),
    ]
    if with_query:
        shapes.append(jax.ShapeDtypeStruct((rows, 128), BF16))
    operands = (o, state, w_own, *fetched, other, gains, *projections)
    return pl.pallas_call(
        body,
        in_specs=[smem()] + [vmem()] * len(operands),
        out_specs=[vmem()] * len(shapes),
        out_shape=shapes,
        compiler_params=PARAMS,
        name="mesh_layer",
    )(meta, *operands)


def final_kernel(meta, counts, o, w_out, grid_in, out):
    tile = grid_in.shape[0]
    heads = jnp.concatenate([o[source(meta, k)] for k in range(MP)], axis=1)
    value = grid_in[...].astype(F32) + dot(heads, w_out[...])
    row = lax.broadcasted_iota(jnp.int32, (BLOCK, 256), 0)
    for b in range(tile // BLOCK):
        count = counts[meta[1] * 8 + pl.program_id(0) * (tile // BLOCK) + b]
        part = value[b * BLOCK : (b + 1) * BLOCK, :]
        out[b * BLOCK : (b + 1) * BLOCK, :] = jnp.where(row < count, part, 0.0).astype(BF16)


def final(meta, counts, o, w_out, grid_in):
    rows = grid_in.shape[0]
    tile = 256
    return pl.pallas_call(
        final_kernel,
        grid=(rows // tile,),
        in_specs=[
            smem(),
            smem(),
            pl.BlockSpec((MP, tile, 128), lambda i: (0, i, 0)),
            vmem(),
            pl.BlockSpec((tile, 256), lambda i: (i, 0)),
        ],
        out_specs=pl.BlockSpec((tile, 256), lambda i: (i, 0)),
        out_shape=jax.ShapeDtypeStruct((rows, 256), BF16),
        compiler_params=PARAMS,
        name="grid_final",
    )(meta, counts, o, w_out, grid_in)


def gather_heads(copies):
    return lax.all_to_all(copies, "mp", split_axis=0, concat_axis=0, tiled=True)


def program(
    grid_in, mesh_in, w_query, w_key, w_value, w_out, norm_gains,
    enc_list, proc_list, dec_list, grid_count,
):
    own_mp, own_node = lax.axis_index("mp"), lax.axis_index("nodes")
    core = own_node % 2
    meta = jnp.concatenate([
        own_mp[None].astype(jnp.int32),
        own_node[None].astype(jnp.int32),
        enc_list.reshape(-1) - (own_node - REACH) * 8,
        proc_list.reshape(-1) - (own_node - REACH) * 2,
        dec_list.reshape(-1) - (own_node - REACH) * 2,
    ])
    gains = norm_gains.reshape(6, MP, 256)

    def gathered(part, name):
        pieces = [part, None, None, None]
        for k in (1, 3, 2):
            pieces[k] = shift_mp(part if name != "w" else part[k], k)
        return pieces

    def window(part):
        pieces = []
        for d in range(-REACH, REACH + 1):
            pieces.append(from_node(part, d) if d else part)
        return pieces

    grid_pieces = gathered(grid_in, "g")
    mesh_pieces = gathered(mesh_in, "m")

    w_groups = w_out.reshape(4, 128, MP, 256).transpose(0, 2, 1, 3)
    own_half = lax.dynamic_slice_in_dim(w_groups[:3], core * 2, 2, axis=1)
    sent = [None] * MP
    for k in (1, 2, 3):
        last = lax.dynamic_index_in_dim(w_groups[3], (own_mp + k) % MP, 0, keepdims=True)
        sent[k] = jnp.concatenate([own_half.reshape(6, 128, 256), last], axis=0)
    sent[0] = sent[1]
    arrived = gathered(sent, "w")[1:]

    kv, grid_q = grid_project(meta, grid_pieces, gains, w_key[0], w_value[0], w_query[3])
    grid_windows = window(kv)
    state, mesh_q = mesh_start(meta, mesh_pieces, gains, w_query[0])
    o = enc_attend(meta, enc_list, grid_count, mesh_q, grid_windows)

    arrived = lax.optimization_barrier((*arrived, o))[:3]
    other = swap_cores(jnp.stack([a[:6] for a in arrived]))
    w_last = jnp.concatenate(
        [lax.dynamic_index_in_dim(w_groups[3], own_mp, 0, keepdims=True)] + [a[6:] for a in arrived], axis=0
    ).reshape(512, 256)

    for index in range(3):
        heads = gather_heads(o)
        projections = [w_key[index + 1], w_value[index + 1]] + ([w_query[index + 1]] if index < 2 else [])
        made = layer(
            index, index + 2 if index < 2 else 5, index < 2, meta, heads, state, w_groups[:3], arrived, other, gains, projections
        )
        state, kv = made[0], made[1]
        near = window(kv)
        if index < 2:
            o = near_attend(PROC0, 3, meta, made[2], near)
    o = near_attend(DEC0, 2, meta, grid_q, near)
    heads = gather_heads(o)
    grid_out = final(meta, grid_count, heads, w_last, grid_in)
    mesh_out = lax.dynamic_index_in_dim(state, own_mp, 0, keepdims=False)
    return grid_out, mesh_out


def solution(mesh):
    placed = (
        P("nodes", "mp"),
        P("nodes", "mp"),
        P(None, None, "mp"),
        P(None, None, "mp"),
        P(None, None, "mp"),
        P(None, "mp", None),
        P(),
        P("nodes", None),
        P("nodes", None),
        P("nodes", None),
        P(),
    )
    return jax.shard_map(
        program,
        mesh=mesh,
        in_specs=placed,
        out_specs=(P("nodes", "mp"), P("nodes", "mp")),
        check_vma=False,
    )
```

```python
import jax
import jax.numpy as jnp
from jax import lax
from jax.experimental import pallas as pl
from jax.experimental.pallas import tpu as pltpu
from jax.sharding import PartitionSpec as P


BLOCK = 128
REACH = 2
EPS = 1e-05
MP = 4
F32 = jnp.float32
BF16 = jnp.bfloat16

ENC0, PROC0, DEC0 = 2, 10, 16


PARAMS = pltpu.CompilerParams(vmem_limit_bytes=16 * 1024 * 1024)


def shift_mp(value, steps):
    return lax.ppermute(value, "mp", [(s, (s + steps) % MP) for s in range(MP)])


def from_node(value, offset):
    count = lax.axis_size("nodes")
    pairs = [(s, s - offset) for s in range(count) if 0 <= s - offset < count]
    return lax.ppermute(value, "nodes", pairs)


def swap_cores(value):
    count = lax.axis_size("nodes")
    return lax.ppermute(value, "nodes", [(s, s ^ 1) for s in range(count)])


def smem():
    return pl.BlockSpec(memory_space=pltpu.SMEM)


def vmem():
    return pl.BlockSpec(memory_space=pltpu.VMEM)


def hbm():
    return pl.BlockSpec(memory_space=pltpu.HBM)


def copies_of(pairs, kept, sems):
    return [
        pltpu.make_async_copy(w.at[layer_index], kept.at[i], sems.at[i])
        for i, (w, layer_index) in enumerate(pairs)
    ]


def source(meta, k):
    return (meta[0] + MP - k) % MP


def normed(pieces):
    width = sum(p.shape[-1] for p in pieces)
    values = [p.astype(F32) for p in pieces]
    mean = sum(jnp.sum(v, axis=-1, keepdims=True) for v in values) * (1.0 / width)
    centred = [v - mean for v in values]
    spread = sum(jnp.sum(c * c, axis=-1, keepdims=True) for c in centred) * (1.0 / width)
    scale = lax.rsqrt(spread + EPS)
    return [c * scale for c in centred]


def dot(a, b):
    return jnp.dot(a, b, preferred_element_type=F32)


def grid_kernel(meta, x0, x1, x2, x3, gains, w_k, w_v, w_q, kv_out, q_out, kept, sems):
    copies = copies_of([(w_k, 0), (w_v, 0), (w_q, 3)], kept, sems)

    @pl.when(pl.program_id(0) == 0)
    def _():
        for copy in copies:
            copy.start()

    rows = normed([x[...] for x in (x0, x1, x2, x3)])

    @pl.when(pl.program_id(0) == 0)
    def _():
        for copy in copies:
            copy.wait()

    kv = q = None
    for k in range(MP):
        src = source(meta, k)
        at = pl.ds(pl.multiple_of(src * 256, 256), 256)
        for_kv = (rows[k] * gains[1, pl.ds(src, 1), :]).astype(BF16)
        for_q = (rows[k] * gains[4, pl.ds(src, 1), :]).astype(BF16)
        kv_part = dot(for_kv, jnp.concatenate([kept[0, at, :], kept[1, at, :]], axis=1))
        q_part = dot(for_q, kept[2, at, :])
        kv = kv_part if kv is None else kv + kv_part
        q = q_part if q is None else q + q_part
    kv_out[...] = kv.astype(BF16)
    q_out[...] = q.astype(BF16)


def grid_project(meta, pieces, gains, w_k, w_v, w_q):
    rows = pieces[0].shape[0]
    tile = 256
    return pl.pallas_call(
        grid_kernel,
        grid=(rows // tile,),
        in_specs=[smem()]
        + [pl.BlockSpec((tile, 256), lambda i: (i, 0))] * MP
        + [vmem(), hbm(), hbm(), hbm()],
        out_specs=[
            pl.BlockSpec((tile, 256), lambda i: (i, 0)),
            pl.BlockSpec((tile, 128), lambda i: (i, 0)),
        ],
        out_shape=[
            jax.ShapeDtypeStruct((rows, 256), BF16),
            jax.ShapeDtypeStruct((rows, 128), BF16),
        ],
        scratch_shapes=[pltpu.VMEM((3, 1024, 128), BF16), pltpu.SemaphoreType.DMA((3,))],
        cost_estimate=pl.CostEstimate(flops=rows * 1024 * 384 * 2, transcendentals=0, bytes_accessed=rows * 4096),
        compiler_params=PARAMS,
        name="grid_project",
    )(meta, *pieces, gains, w_k, w_v, w_q)


def mesh_kernel(meta, x0, a1, a2, a3, gains, w_q, q_out, kept, sems):
    copies = copies_of([(w_q, 0)], kept, sems)
    copies[0].start()
    rows = normed([x0[...]] + [a[...].reshape(2 * BLOCK, 256) for a in (a1, a2, a3)])
    copies[0].wait()
    q = None
    for k in range(MP):
        src = source(meta, k)
        at = pl.ds(pl.multiple_of(src * 256, 256), 256)
        part = dot((rows[k] * gains[0, pl.ds(src, 1), :]).astype(BF16), kept[0, at, :])
        q = part if q is None else q + part
    q_out[...] = q.astype(BF16)


def mesh_start(meta, mesh_in, arrived, gains, w_q):
    rows = mesh_in.shape[0]
    return pl.pallas_call(
        mesh_kernel,
        grid=(1,),
        in_specs=[smem(), vmem()]
        + [pl.BlockSpec((2, BLOCK, 256), lambda i: (0, 0, 0))] * 3
        + [vmem(), hbm()],
        out_specs=vmem(),
        out_shape=jax.ShapeDtypeStruct((rows, 128), BF16),
        scratch_shapes=[pltpu.VMEM((1, 1024, 128), BF16), pltpu.SemaphoreType.DMA((1,))],
        cost_estimate=pl.CostEstimate(flops=rows * 1024 * 128 * 2, transcendentals=0, bytes_accessed=rows * 4096),
        compiler_params=PARAMS,
        name="mesh_start",
    )(meta, mesh_in, *arrived, gains, w_q)


def head_rows():
    lane = lax.broadcasted_iota(jnp.int32, (1, 128), 1)
    first = jnp.where(lane < 64, 0.125, 0.0).astype(BF16)
    second = jnp.where(lane < 64, 0.0, 0.125).astype(BF16)
    return first, second


def attend_block(q, keys, values, key_ok):
    outs = []
    for row in head_rows():
        scores = lax.dot_general(
            q * row, keys, (((1,), (1,)), ((), ())), preferred_element_type=F32
        )
        if key_ok is not None:
            scores = jnp.where(key_ok, scores, -1e30)
        highest = jnp.max(scores, axis=-1, keepdims=True)
        weights = jnp.exp(scores - highest)
        total = jnp.sum(weights, axis=-1, keepdims=True)
        outs.append(dot(weights.astype(BF16), values) / total)
    lane = lax.broadcasted_iota(jnp.int32, outs[0].shape, 1)
    return jnp.where(lane < 64, outs[0], outs[1]).astype(BF16)


def enc_kernel(meta, listed, counts, q, *rest):
    windows, o_out, kept = rest[:-2], rest[-2], rest[-1]
    blocks_each = windows[0].shape[0] // BLOCK
    for slot in range(8):
        place = meta[ENC0 + slot]
        which = place // blocks_each
        start = pl.multiple_of((place % blocks_each) * BLOCK, BLOCK)
        for i, array in enumerate(windows):

            @pl.when(which == i)
            def _():
                kept[slot] = array[pl.ds(start, BLOCK), :]

    lane = lax.broadcasted_iota(jnp.int32, (1, BLOCK), 1)
    for b in range(2):
        key_ok = jnp.concatenate(
            [lane < counts[listed[b, j]] for j in range(4)], axis=1
        )
        kv = kept[b * 4 : b * 4 + 4].reshape(4 * BLOCK, 256)
        o = attend_block(q[b * BLOCK : (b + 1) * BLOCK, :], kv[:, :128], kv[:, 128:], key_ok)
        for j in range(MP):
            o_out[j, b * BLOCK : (b + 1) * BLOCK, :] = o


def enc_attend(meta, listed, counts, q, windows):
    return pl.pallas_call(
        enc_kernel,
        in_specs=[smem(), smem(), smem()] + [vmem()] * (1 + len(windows)),
        out_specs=vmem(),
        out_shape=jax.ShapeDtypeStruct((MP,) + q.shape, BF16),
        scratch_shapes=[pltpu.VMEM((8, BLOCK, 256), BF16)],
        compiler_params=PARAMS,
        name="enc_attend",
    )(meta, listed, counts, q, *windows)


def near_kernel(first_entry, per_block, meta, q, a0, a1, a2, a3, a4, o_out, kept):
    for i, array in enumerate((a0, a1, a2, a3, a4)):
        kept[2 * i] = array[0:BLOCK, :]
        kept[2 * i + 1] = array[BLOCK : 2 * BLOCK, :]
    for b in range(q.shape[0] // BLOCK):
        kv = jnp.concatenate(
            [kept[meta[first_entry + b * per_block + j]] for j in range(per_block)], axis=0
        )
        o = attend_block(q[b * BLOCK : (b + 1) * BLOCK, :], kv[:, :128], kv[:, 128:], None)
        for j in range(MP):
            o_out[j, b * BLOCK : (b + 1) * BLOCK, :] = o


def near_attend(first_entry, per_block, meta, q, windows):
    def body(*refs):
        near_kernel(first_entry, per_block, *refs)

    return pl.pallas_call(
        body,
        in_specs=[smem()] + [vmem()] * 6,
        out_specs=vmem(),
        out_shape=jax.ShapeDtypeStruct((MP,) + q.shape, BF16),
        scratch_shapes=[pltpu.VMEM((10, BLOCK, 256), BF16)],
        compiler_params=PARAMS,
        name="near_attend",
    )(meta, q, *windows)


def layer_kernel(index, gain_row, meta, o, state, w_own, a1, a2, a3, other, gains, w_k, w_v, w_q, *rest):
    last = index == 2
    state_out, kv_out = rest[0], rest[1]
    new, kept, sems = rest[2 + (not last) :]
    weights = (w_k, w_v) if last else (w_k, w_v, w_q)
    copies = copies_of([(w, index + 1) for w in weights], kept, sems)
    for copy in copies:
        copy.start()
    if index == 0:
        new[meta[0]] = state[...]
        for k, a in enumerate((a1, a2, a3)):
            new[source(meta, k + 1)] = a[0:2].reshape(2 * BLOCK, 256)
        state = new
    heads = jnp.concatenate([o[source(meta, k)] for k in range(MP)], axis=1)
    core = meta[1] % 2
    for part in range(4):
        at = index + 3 * (part % 2)
        if part < 2:
            g = 2 * core + part
            fetched = [a[2 + at] for a in (a1, a2, a3)]
        else:
            g = 2 * (1 - core) + part - 2
            fetched = [other[k, at] for k in range(MP - 1)]
        own = w_own[index, :, pl.ds(pl.multiple_of(g * 256, 256), 256)]
        w_out = jnp.concatenate([own] + fetched, axis=0)
        new[g] = (state[g].astype(F32) + dot(heads, w_out)).astype(BF16)
    if last:
        state_out[...] = new[meta[0]]
    else:
        for g in range(MP):
            state_out[g] = new[g]
    rows = normed([new[g] for g in range(MP)])
    row = jnp.concatenate(
        [(rows[g] * gains[gain_row, g : g + 1, :]).astype(BF16) for g in range(MP)], axis=1
    )
    for copy in copies:
        copy.wait()
    result = dot(row, jnp.concatenate([kept[i] for i in range(len(weights))], axis=1)).astype(BF16)
    kv_out[...] = result[:, :256]
    if not last:
        rest[2][...] = result[:, 256:]


def layer(index, gain_row, meta, o, state, w_own, fetched, other, gains, w_key, w_value, w_query):
    def body(*refs):
        layer_kernel(index, gain_row, *refs)

    last = index == 2
    rows = o.shape[1]
    shapes = [
        jax.ShapeDtypeStruct((rows, 256) if last else (MP, rows, 256), BF16),
        jax.ShapeDtypeStruct((rows, 256), BF16),
    ]
    if not last:
        shapes.append(jax.ShapeDtypeStruct((rows, 128), BF16))
    operands = (o, state, w_own, *fetched, other, gains)
    return pl.pallas_call(
        body,
        in_specs=[smem()] + [vmem()] * len(operands) + [hbm()] * 3,
        out_specs=[vmem()] * len(shapes),
        out_shape=shapes,
        scratch_shapes=[
            pltpu.VMEM((MP, rows, 256), BF16),
            pltpu.VMEM((3, 1024, 128), BF16),
            pltpu.SemaphoreType.DMA((3,)),
        ],
        compiler_params=PARAMS,
        name="mesh_layer",
    )(meta, *operands, w_key, w_value, w_query)


def final_kernel(meta, counts, o, w_out, grid_in, out):
    tile = grid_in.shape[0]
    heads = jnp.concatenate([o[source(meta, k)] for k in range(MP)], axis=1)
    value = grid_in[...].astype(F32) + dot(heads, w_out[...])
    row = lax.broadcasted_iota(jnp.int32, (BLOCK, 256), 0)
    for b in range(tile // BLOCK):
        count = counts[meta[1] * 8 + pl.program_id(0) * (tile // BLOCK) + b]
        part = value[b * BLOCK : (b + 1) * BLOCK, :]
        out[b * BLOCK : (b + 1) * BLOCK, :] = jnp.where(row < count, part, 0.0).astype(BF16)


def final(meta, counts, o, w_out, grid_in):
    rows = grid_in.shape[0]
    tile = 256
    return pl.pallas_call(
        final_kernel,
        grid=(rows // tile,),
        in_specs=[
            smem(),
            smem(),
            pl.BlockSpec((MP, tile, 128), lambda i: (0, i, 0)),
            vmem(),
            pl.BlockSpec((tile, 256), lambda i: (i, 0)),
        ],
        out_specs=pl.BlockSpec((tile, 256), lambda i: (i, 0)),
        out_shape=jax.ShapeDtypeStruct((rows, 256), BF16),
        compiler_params=PARAMS,
        name="grid_final",
    )(meta, counts, o, w_out, grid_in)


def gather_heads(copies):
    return lax.all_to_all(copies, "mp", split_axis=0, concat_axis=0, tiled=True)


def program(
    grid_in, mesh_in, w_query, w_key, w_value, w_out, norm_gains,
    enc_list, proc_list, dec_list, grid_count,
):
    own_mp, own_node = lax.axis_index("mp"), lax.axis_index("nodes")
    core = own_node % 2
    meta = jnp.concatenate([
        own_mp[None].astype(jnp.int32),
        own_node[None].astype(jnp.int32),
        enc_list.reshape(-1) - (own_node - REACH) * 8,
        proc_list.reshape(-1) - (own_node - REACH) * 2,
        dec_list.reshape(-1) - (own_node - REACH) * 2,
    ])
    gains = norm_gains.reshape(6, MP, 256)
    w_query, w_key, w_value = (
        pltpu.with_memory_space_constraint(w, pltpu.HBM) for w in (w_query, w_key, w_value)
    )

    def gathered(part, name):
        pieces = [part, None, None, None]
        for k in (1, 3, 2):
            pieces[k] = shift_mp(part if name != "w" else part[k], k)
        return pieces

    def window(part):
        pieces = []
        for d in range(-REACH, REACH + 1):
            pieces.append(from_node(part, d) if d else part)
        return pieces

    grid_pieces = gathered(grid_in, "g")
    grid_pieces[0] = pltpu.with_memory_space_constraint(grid_in, pltpu.HBM)

    halves = [lax.dynamic_slice_in_dim(w_out[:3], core * 512 + part * 256, 256, axis=2) for part in range(2)]
    sent = [None] * MP
    for k in (1, 2, 3):
        last = lax.dynamic_slice_in_dim(w_out[3:], (own_mp + k) % MP * 256, 256, axis=2)
        sent[k] = jnp.concatenate([mesh_in.reshape(2, BLOCK, 256)] + halves + [last], axis=0)
    sent[0] = sent[1]
    arrived = gathered(sent, "w")[1:]

    kv, grid_q = grid_project(meta, grid_pieces, gains, w_key, w_value, w_query)
    grid_windows = window(kv)
    mesh_q = mesh_start(meta, mesh_in, arrived, gains, w_query)
    o = enc_attend(meta, enc_list, grid_count, mesh_q, grid_windows)

    arrived = lax.optimization_barrier((*arrived, o))[:3]
    other = swap_cores(jnp.stack([a[2:8] for a in arrived]))
    w_last = jnp.concatenate(
        [lax.dynamic_slice_in_dim(w_out[3:], own_mp * 256, 256, axis=2)] + [a[8:] for a in arrived], axis=0
    ).reshape(512, 256)

    state = mesh_in
    for index in range(3):
        heads = gather_heads(o)
        made = layer(
            index, index + 2 if index < 2 else 5, meta, heads, state, w_out, arrived, other, gains, w_key, w_value, w_query
        )
        state, kv = made[0], made[1]
        near = window(kv)
        if index < 2:
            o = near_attend(PROC0, 3, meta, made[2], near)
    o = near_attend(DEC0, 2, meta, grid_q, near)
    heads = gather_heads(o)
    grid_out = final(meta, grid_count, heads, w_last, grid_in)
    return grid_out, state


def solution(mesh):
    placed = (
        P("nodes", "mp"),
        P("nodes", "mp"),
        P(None, None, "mp"),
        P(None, None, "mp"),
        P(None, None, "mp"),
        P(None, "mp", None),
        P(),
        P("nodes", None),
        P("nodes", None),
        P("nodes", None),
        P(),
    )
    return jax.shard_map(
        program,
        mesh=mesh,
        in_specs=placed,
        out_specs=(P("nodes", "mp"), P("nodes", "mp")),
        check_vma=False,
    )
```

```python
import jax
import jax.numpy as jnp
from jax import lax
from jax.experimental import pallas as pl
from jax.experimental.pallas import tpu as pltpu
from jax.sharding import PartitionSpec as P


BLOCK = 128
REACH = 2
EPS = 1e-05
MP = 4
F32 = jnp.float32
BF16 = jnp.bfloat16

ENC0, PROC0, DEC0 = 2, 10, 16


PARAMS = pltpu.CompilerParams(vmem_limit_bytes=16 * 1024 * 1024)


def shift_mp(value, steps):
    return lax.ppermute(value, "mp", [(s, (s + steps) % MP) for s in range(MP)])


def from_node(value, offset):
    count = lax.axis_size("nodes")
    pairs = [(s, s - offset) for s in range(count) if 0 <= s - offset < count]
    return lax.ppermute(value, "nodes", pairs)


def swap_cores(value):
    count = lax.axis_size("nodes")
    return lax.ppermute(value, "nodes", [(s, s ^ 1) for s in range(count)])


def smem():
    return pl.BlockSpec(memory_space=pltpu.SMEM)


def vmem():
    return pl.BlockSpec(memory_space=pltpu.VMEM)


def hbm():
    return pl.BlockSpec(memory_space=pltpu.HBM)


def copies_of(pairs, kept, sems):
    return [
        pltpu.make_async_copy(w.at[layer_index], kept.at[i], sems.at[i])
        for i, (w, layer_index) in enumerate(pairs)
    ]


def source(meta, k):
    return (meta[0] + MP - k) % MP


def normed(pieces):
    width = sum(p.shape[-1] for p in pieces)
    values = [p.astype(F32) for p in pieces]
    mean = sum(jnp.sum(v, axis=-1, keepdims=True) for v in values) * (1.0 / width)
    centred = [v - mean for v in values]
    spread = sum(jnp.sum(c * c, axis=-1, keepdims=True) for c in centred) * (1.0 / width)
    scale = lax.rsqrt(spread + EPS)
    return [c * scale for c in centred]


def dot(a, b):
    return jnp.dot(a, b, preferred_element_type=F32)


def grid_kernel(meta, x0, x1, x2, x3, gains, w_k, w_v, w_q, kv_out, q_out, kept, sems):
    copies = copies_of([(w_k, 0), (w_v, 0), (w_q, 3)], kept, sems)

    @pl.when(pl.program_id(0) == 0)
    def _():
        for copy in copies:
            copy.start()

    rows = normed([x[...] for x in (x0, x1, x2, x3)])

    @pl.when(pl.program_id(0) == 0)
    def _():
        for copy in copies:
            copy.wait()

    kv = q = None
    for k in range(MP):
        src = source(meta, k)
        at = pl.ds(pl.multiple_of(src * 256, 256), 256)
        for_kv = (rows[k] * gains[1, pl.ds(src, 1), :]).astype(BF16)
        for_q = (rows[k] * gains[4, pl.ds(src, 1), :]).astype(BF16)
        kv_part = dot(for_kv, jnp.concatenate([kept[0, at, :], kept[1, at, :]], axis=1))
        q_part = dot(for_q, kept[2, at, :])
        kv = kv_part if kv is None else kv + kv_part
        q = q_part if q is None else q + q_part
    kv_out[...] = kv.astype(BF16)
    q_out[...] = q.astype(BF16)


def grid_project(meta, pieces, gains, w_k, w_v, w_q):
    rows = pieces[0].shape[0]
    tile = 256
    return pl.pallas_call(
        grid_kernel,
        grid=(rows // tile,),
        in_specs=[smem()]
        + [pl.BlockSpec((tile, 256), lambda i: (i, 0))] * MP
        + [vmem(), hbm(), hbm(), hbm()],
        out_specs=[
            pl.BlockSpec((tile, 256), lambda i: (i, 0)),
            pl.BlockSpec((tile, 128), lambda i: (i, 0)),
        ],
        out_shape=[
            jax.ShapeDtypeStruct((rows, 256), BF16),
            jax.ShapeDtypeStruct((rows, 128), BF16),
        ],
        scratch_shapes=[pltpu.VMEM((3, 1024, 128), BF16), pltpu.SemaphoreType.DMA((3,))],
        cost_estimate=pl.CostEstimate(flops=rows * 1024 * 384 * 2, transcendentals=0, bytes_accessed=rows * 4096),
        compiler_params=PARAMS,
        name="grid_project",
    )(meta, *pieces, gains, w_k, w_v, w_q)


def mesh_kernel(meta, x0, a1, a2, a3, gains, w_q, q_out, kept, sems):
    copies = copies_of([(w_q, 0)], kept, sems)
    copies[0].start()
    rows = normed([x0[...]] + [a[...].reshape(2 * BLOCK, 256) for a in (a1, a2, a3)])
    copies[0].wait()
    q = None
    for k in range(MP):
        src = source(meta, k)
        at = pl.ds(pl.multiple_of(src * 256, 256), 256)
        part = dot((rows[k] * gains[0, pl.ds(src, 1), :]).astype(BF16), kept[0, at, :])
        q = part if q is None else q + part
    q_out[...] = q.astype(BF16)


def mesh_start(meta, mesh_in, arrived, gains, w_q):
    rows = mesh_in.shape[0]
    return pl.pallas_call(
        mesh_kernel,
        grid=(1,),
        in_specs=[smem(), vmem()]
        + [pl.BlockSpec((2, BLOCK, 256), lambda i: (0, 0, 0))] * 3
        + [vmem(), hbm()],
        out_specs=vmem(),
        out_shape=jax.ShapeDtypeStruct((rows, 128), BF16),
        scratch_shapes=[pltpu.VMEM((1, 1024, 128), BF16), pltpu.SemaphoreType.DMA((1,))],
        cost_estimate=pl.CostEstimate(flops=rows * 1024 * 128 * 2, transcendentals=0, bytes_accessed=rows * 4096),
        compiler_params=PARAMS,
        name="mesh_start",
    )(meta, mesh_in, *arrived, gains, w_q)


def head_rows():
    lane = lax.broadcasted_iota(jnp.int32, (1, 128), 1)
    first = jnp.where(lane < 64, 0.125, 0.0).astype(BF16)
    second = jnp.where(lane < 64, 0.0, 0.125).astype(BF16)
    return first, second


def attend_block(q, keys, values, key_ok):
    outs = []
    for row in head_rows():
        scores = lax.dot_general(
            q * row, keys, (((1,), (1,)), ((), ())), preferred_element_type=F32
        )
        if key_ok is not None:
            scores = jnp.where(key_ok, scores, -1e30)
        highest = jnp.max(scores, axis=-1, keepdims=True)
        weights = jnp.exp(scores - highest)
        total = jnp.sum(weights, axis=-1, keepdims=True)
        outs.append(dot(weights.astype(BF16), values) / total)
    lane = lax.broadcasted_iota(jnp.int32, outs[0].shape, 1)
    return jnp.where(lane < 64, outs[0], outs[1]).astype(BF16)


def window_places(meta):
    core = meta[1] % 2
    return 0, 2, 4, 3 - 2 * core, 1 + 2 * core


def enc_kernel(meta, listed, counts, q, a0, a1, a2, a3, a4, o_out, kept):
    blocks_each = a0.shape[0] // BLOCK
    places = window_places(meta)
    for slot in range(8):
        place = meta[ENC0 + slot]
        which = place // blocks_each
        start = pl.multiple_of((place % blocks_each) * BLOCK, BLOCK)
        for w, array in zip(places, (a0, a1, a2, a3, a4)):

            @pl.when(which == w)
            def _():
                kept[slot] = array[pl.ds(start, BLOCK), :]

    lane = lax.broadcasted_iota(jnp.int32, (1, BLOCK), 1)
    for b in range(2):
        key_ok = jnp.concatenate(
            [lane < counts[listed[b, j]] for j in range(4)], axis=1
        )
        kv = kept[b * 4 : b * 4 + 4].reshape(4 * BLOCK, 256)
        o = attend_block(q[b * BLOCK : (b + 1) * BLOCK, :], kv[:, :128], kv[:, 128:], key_ok)
        for j in range(MP):
            o_out[j, b * BLOCK : (b + 1) * BLOCK, :] = o


def enc_attend(meta, listed, counts, q, windows):
    return pl.pallas_call(
        enc_kernel,
        in_specs=[smem(), smem(), smem()] + [vmem()] * 6,
        out_specs=vmem(),
        out_shape=jax.ShapeDtypeStruct((MP,) + q.shape, BF16),
        scratch_shapes=[pltpu.VMEM((8, BLOCK, 256), BF16)],
        compiler_params=PARAMS,
        name="enc_attend",
    )(meta, listed, counts, q, *windows)


def near_kernel(first_entry, per_block, meta, q, a0, a1, a2, a3, a4, o_out, kept):
    for w, array in zip(window_places(meta), (a0, a1, a2, a3, a4)):
        kept[2 * w] = array[0:BLOCK, :]
        kept[2 * w + 1] = array[BLOCK : 2 * BLOCK, :]
    for b in range(q.shape[0] // BLOCK):
        kv = jnp.concatenate(
            [kept[meta[first_entry + b * per_block + j]] for j in range(per_block)], axis=0
        )
        o = attend_block(q[b * BLOCK : (b + 1) * BLOCK, :], kv[:, :128], kv[:, 128:], None)
        for j in range(MP):
            o_out[j, b * BLOCK : (b + 1) * BLOCK, :] = o


def near_attend(first_entry, per_block, meta, q, windows):
    def body(*refs):
        near_kernel(first_entry, per_block, *refs)

    return pl.pallas_call(
        body,
        in_specs=[smem()] + [vmem()] * 6,
        out_specs=vmem(),
        out_shape=jax.ShapeDtypeStruct((MP,) + q.shape, BF16),
        scratch_shapes=[pltpu.VMEM((10, BLOCK, 256), BF16)],
        compiler_params=PARAMS,
        name="near_attend",
    )(meta, q, *windows)


def layer_kernel(index, gain_row, meta, o, state, a1, a2, a3, gains, w_own, b1, b2, b3, other, w_k, w_v, w_q, *rest):
    last = index == 2
    state_out, kv_out = rest[0], rest[1]
    new, w_out, kept, w_sems, sems = rest[2 + (not last) :]
    core = meta[1] % 2
    for g in range(MP):
        pltpu.make_async_copy(
            w_own.at[index, :, g * 256 : (g + 1) * 256], w_out.at[g, 0:BLOCK, :], w_sems.at[g, 0]
        ).start()
    for part in range(2):
        at = index + 3 * part
        for k, b in enumerate((b1, b2, b3)):
            rows = w_out.at[2 * core + part, (k + 1) * BLOCK : (k + 2) * BLOCK, :]
            pltpu.make_async_copy(b.at[2 + at], rows, w_sems.at[2 * core + part, k + 1]).start()
            rows = w_out.at[2 * (1 - core) + part, (k + 1) * BLOCK : (k + 2) * BLOCK, :]
            pltpu.make_async_copy(other.at[k, at], rows, w_sems.at[2 * (1 - core) + part, k + 1]).start()
    weights = (w_k, w_v) if last else (w_k, w_v, w_q)
    copies = copies_of([(w, index + 1) for w in weights], kept, sems)
    for copy in copies:
        copy.start()
    if index == 0:
        new[meta[0]] = state[...]
        for k, a in enumerate((a1, a2, a3)):
            new[source(meta, k + 1)] = a[...].reshape(2 * BLOCK, 256)
        state = new
    heads = jnp.concatenate([o[source(meta, k)] for k in range(MP)], axis=1)
    for g in range(MP):
        for k in range(MP):
            rows = w_out.at[g, k * BLOCK : (k + 1) * BLOCK, :]
            pltpu.make_async_copy(other.at[0, 0], rows, w_sems.at[g, k]).wait()
        new[g] = (state[g].astype(F32) + dot(heads, w_out[g])).astype(BF16)
    if last:
        state_out[...] = new[meta[0]]
    else:
        for g in range(MP):
            state_out[g] = new[g]
    rows = normed([new[g] for g in range(MP)])
    row = jnp.concatenate(
        [(rows[g] * gains[gain_row, g : g + 1, :]).astype(BF16) for g in range(MP)], axis=1
    )
    for copy in copies:
        copy.wait()
    result = dot(row, jnp.concatenate([kept[i] for i in range(len(weights))], axis=1)).astype(BF16)
    kv_out[...] = result[:, :256]
    if not last:
        rest[2][...] = result[:, 256:]


def layer(index, gain_row, meta, o, state, w_own, fetched, other, gains, w_key, w_value, w_query):
    def body(*refs):
        layer_kernel(index, gain_row, *refs)

    last = index == 2
    rows = o.shape[1]
    shapes = [
        jax.ShapeDtypeStruct((rows, 256) if last else (MP, rows, 256), BF16),
        jax.ShapeDtypeStruct((rows, 256), BF16),
    ]
    if not last:
        shapes.append(jax.ShapeDtypeStruct((rows, 128), BF16))
    return pl.pallas_call(
        body,
        grid=(1,),
        in_specs=[smem(), vmem(), vmem()]
        + [pl.BlockSpec((2, BLOCK, 256), lambda i: (0, 0, 0))] * 3
        + [vmem()]
        + [hbm()] * 8,
        out_specs=[vmem()] * len(shapes),
        out_shape=shapes,
        scratch_shapes=[
            pltpu.VMEM((MP, rows, 256), BF16),
            pltpu.VMEM((MP, 4 * BLOCK, 256), BF16),
            pltpu.VMEM((3, 1024, 128), BF16),
            pltpu.SemaphoreType.DMA((MP, MP)),
            pltpu.SemaphoreType.DMA((3,)),
        ],
        compiler_params=PARAMS,
        name="mesh_layer",
    )(meta, o, state, *fetched, gains, w_own, *fetched, other, w_key, w_value, w_query)


def final_kernel(meta, counts, o, w_out, grid_in, out):
    tile = grid_in.shape[0]
    heads = jnp.concatenate([o[source(meta, k)] for k in range(MP)], axis=1)
    value = grid_in[...].astype(F32) + dot(heads, w_out[...])
    row = lax.broadcasted_iota(jnp.int32, (BLOCK, 256), 0)
    for b in range(tile // BLOCK):
        count = counts[meta[1] * 8 + pl.program_id(0) * (tile // BLOCK) + b]
        part = value[b * BLOCK : (b + 1) * BLOCK, :]
        out[b * BLOCK : (b + 1) * BLOCK, :] = jnp.where(row < count, part, 0.0).astype(BF16)


def final(meta, counts, o, w_out, grid_in):
    rows = grid_in.shape[0]
    tile = 512
    return pl.pallas_call(
        final_kernel,
        grid=(rows // tile,),
        in_specs=[
            smem(),
            smem(),
            pl.BlockSpec((MP, tile, 128), lambda i: (0, i, 0)),
            vmem(),
            pl.BlockSpec((tile, 256), lambda i: (i, 0)),
        ],
        out_specs=pl.BlockSpec((tile, 256), lambda i: (i, 0)),
        out_shape=jax.ShapeDtypeStruct((rows, 256), BF16),
        compiler_params=PARAMS,
        name="grid_final",
    )(meta, counts, o, w_out, grid_in)


def gather_heads(copies):
    return lax.all_to_all(copies, "mp", split_axis=0, concat_axis=0, tiled=True)


def program(
    grid_in, mesh_in, w_query, w_key, w_value, w_out, norm_gains,
    enc_list, proc_list, dec_list, grid_count,
):
    own_mp, own_node = lax.axis_index("mp"), lax.axis_index("nodes")
    core = own_node % 2
    meta = jnp.concatenate([
        own_mp[None].astype(jnp.int32),
        own_node[None].astype(jnp.int32),
        enc_list.reshape(-1) - (own_node - REACH) * 8,
        proc_list.reshape(-1) - (own_node - REACH) * 2,
        dec_list.reshape(-1) - (own_node - REACH) * 2,
    ])
    gains = norm_gains.reshape(6, MP, 256)
    w_query, w_key, w_value = (
        pltpu.with_memory_space_constraint(w, pltpu.HBM) for w in (w_query, w_key, w_value)
    )

    def gathered(part, name):
        pieces = [part, None, None, None]
        for k in (1, 3, 2):
            pieces[k] = shift_mp(part if name != "w" else part[k], k)
        return pieces

    def window(part):
        low = from_node(part, -2)
        high = from_node(part, 2)
        beside = swap_cores(part)
        beyond = swap_cores(jnp.where(core == 0, high, low))
        return [low, part, high, beside, beyond]

    grid_pieces = gathered(grid_in, "g")
    grid_pieces[0] = pltpu.with_memory_space_constraint(grid_in, pltpu.HBM)

    halves = [lax.dynamic_slice_in_dim(w_out[:3], core * 512 + part * 256, 256, axis=2) for part in range(2)]
    sent = [None] * MP
    for k in (1, 2, 3):
        last = lax.dynamic_slice_in_dim(w_out[3:], (own_mp + k) % MP * 256, 256, axis=2)
        sent[k] = jnp.concatenate([mesh_in.reshape(2, BLOCK, 256)] + halves + [last], axis=0)
    sent[0] = sent[1]
    arrived = gathered(sent, "w")[1:]

    kv, grid_q = grid_project(meta, grid_pieces, gains, w_key, w_value, w_query)
    grid_windows = window(kv)
    mesh_q = mesh_start(meta, mesh_in, arrived, gains, w_query)
    o = enc_attend(meta, enc_list, grid_count, mesh_q, grid_windows)

    arrived = lax.optimization_barrier((*arrived, o))[:3]
    other = swap_cores(jnp.stack([a[2:8] for a in arrived]))
    other = pltpu.with_memory_space_constraint(other, pltpu.HBM)
    w_own = pltpu.with_memory_space_constraint(w_out, pltpu.HBM)
    w_last = jnp.concatenate(
        [lax.dynamic_slice_in_dim(w_out[3:], own_mp * 256, 256, axis=2)] + [a[8:] for a in arrived], axis=0
    ).reshape(512, 256)

    state = mesh_in
    for index in range(3):
        heads = gather_heads(o)
        made = layer(
            index, index + 2 if index < 2 else 5, meta, heads, state, w_own, arrived, other, gains, w_key, w_value, w_query
        )
        state, kv = made[0], made[1]
        near = window(kv)
        if index < 2:
            o = near_attend(PROC0, 3, meta, made[2], near)
    o = near_attend(DEC0, 2, meta, grid_q, near)
    heads = gather_heads(o)
    grid_out = final(meta, grid_count, heads, w_last, grid_in)
    return grid_out, state


def solution(mesh):
    placed = (
        P("nodes", "mp"),
        P("nodes", "mp"),
        P(None, None, "mp"),
        P(None, None, "mp"),
        P(None, None, "mp"),
        P(None, "mp", None),
        P(),
        P("nodes", None),
        P("nodes", None),
        P("nodes", None),
        P(),
    )
    return jax.shard_map(
        program,
        mesh=mesh,
        in_specs=placed,
        out_specs=(P("nodes", "mp"), P("nodes", "mp")),
        check_vma=False,
    )
```

```python
import jax
import jax.numpy as jnp
from jax import lax
from jax.experimental import pallas as pl
from jax.experimental.pallas import tpu as pltpu
from jax.sharding import PartitionSpec as P


BLOCK = 128
REACH = 2
EPS = 1e-05
MP = 4
F32 = jnp.float32
BF16 = jnp.bfloat16

ENC0, PROC0, DEC0 = 2, 10, 16


PARAMS = pltpu.CompilerParams(vmem_limit_bytes=16 * 1024 * 1024)


def shift_mp(value, steps):
    return lax.ppermute(value, "mp", [(s, (s + steps) % MP) for s in range(MP)])


def from_node(value, offset):
    count = lax.axis_size("nodes")
    pairs = [(s, s - offset) for s in range(count) if 0 <= s - offset < count]
    return lax.ppermute(value, "nodes", pairs)


def swap_cores(value):
    count = lax.axis_size("nodes")
    return lax.ppermute(value, "nodes", [(s, s ^ 1) for s in range(count)])


def smem():
    return pl.BlockSpec(memory_space=pltpu.SMEM)


def vmem():
    return pl.BlockSpec(memory_space=pltpu.VMEM)


def hbm():
    return pl.BlockSpec(memory_space=pltpu.HBM)


def copies_of(pairs, kept, sems):
    return [
        pltpu.make_async_copy(w.at[layer_index], kept.at[i], sems.at[i])
        for i, (w, layer_index) in enumerate(pairs)
    ]


def source(meta, k):
    return (meta[0] + MP - k) % MP


def normed(pieces):
    width = sum(p.shape[-1] for p in pieces)
    values = [p.astype(F32) for p in pieces]
    mean = sum(jnp.sum(v, axis=-1, keepdims=True) for v in values) * (1.0 / width)
    centred = [v - mean for v in values]
    spread = sum(jnp.sum(c * c, axis=-1, keepdims=True) for c in centred) * (1.0 / width)
    scale = lax.rsqrt(spread + EPS)
    return [c * scale for c in centred]


def dot(a, b):
    return jnp.dot(a, b, preferred_element_type=F32)


def grid_kernel(gain_row, count, layer_index, meta, x0, x1, x2, x3, gains, *rest):
    weights, (out, kept, sems) = rest[:count], rest[count:]
    copies = copies_of([(w, layer_index) for w in weights], kept, sems)

    @pl.when(pl.program_id(0) == 0)
    def _():
        for copy in copies:
            copy.start()

    rows = normed([x[...] for x in (x0, x1, x2, x3)])

    @pl.when(pl.program_id(0) == 0)
    def _():
        for copy in copies:
            copy.wait()

    total = None
    for k in range(MP):
        src = source(meta, k)
        at = pl.ds(pl.multiple_of(src * 256, 256), 256)
        row = (rows[k] * gains[gain_row, pl.ds(src, 1), :]).astype(BF16)
        part = dot(row, jnp.concatenate([kept[i, at, :] for i in range(count)], axis=1))
        total = part if total is None else total + part
    out[...] = total.astype(BF16)


def grid_project(gain_row, layer_index, meta, pieces, gains, *weights):
    count = len(weights)

    def body(*refs):
        grid_kernel(gain_row, count, layer_index, *refs)

    rows = pieces[0].shape[0]
    tile = 256
    return pl.pallas_call(
        body,
        grid=(rows // tile,),
        in_specs=[smem()]
        + [pl.BlockSpec((tile, 256), lambda i: (i, 0))] * MP
        + [vmem()]
        + [hbm()] * count,
        out_specs=pl.BlockSpec((tile, 128 * count), lambda i: (i, 0)),
        out_shape=jax.ShapeDtypeStruct((rows, 128 * count), BF16),
        scratch_shapes=[pltpu.VMEM((count, 1024, 128), BF16), pltpu.SemaphoreType.DMA((count,))],
        cost_estimate=pl.CostEstimate(flops=rows * 1024 * 128 * count * 2, transcendentals=0, bytes_accessed=rows * 4096),
        compiler_params=PARAMS,
        name="grid_project",
    )(meta, *pieces, gains, *weights)


def mesh_kernel(meta, x0, a1, a2, a3, gains, w_q, q_out, kept, sems):
    copies = copies_of([(w_q, 0)], kept, sems)
    copies[0].start()
    rows = normed([x0[...]] + [a[...].reshape(2 * BLOCK, 256) for a in (a1, a2, a3)])
    copies[0].wait()
    q = None
    for k in range(MP):
        src = source(meta, k)
        at = pl.ds(pl.multiple_of(src * 256, 256), 256)
        part = dot((rows[k] * gains[0, pl.ds(src, 1), :]).astype(BF16), kept[0, at, :])
        q = part if q is None else q + part
    q_out[...] = q.astype(BF16)


def mesh_start(meta, mesh_in, arrived, gains, w_q):
    rows = mesh_in.shape[0]
    return pl.pallas_call(
        mesh_kernel,
        grid=(1,),
        in_specs=[smem(), vmem()]
        + [pl.BlockSpec((2, BLOCK, 256), lambda i: (0, 0, 0))] * 3
        + [vmem(), hbm()],
        out_specs=vmem(),
        out_shape=jax.ShapeDtypeStruct((rows, 128), BF16),
        scratch_shapes=[pltpu.VMEM((1, 1024, 128), BF16), pltpu.SemaphoreType.DMA((1,))],
        cost_estimate=pl.CostEstimate(flops=rows * 1024 * 128 * 2, transcendentals=0, bytes_accessed=rows * 4096),
        compiler_params=PARAMS,
        name="mesh_start",
    )(meta, mesh_in, *arrived, gains, w_q)


def head_rows():
    lane = lax.broadcasted_iota(jnp.int32, (1, 128), 1)
    first = jnp.where(lane < 64, 0.125, 0.0).astype(BF16)
    second = jnp.where(lane < 64, 0.0, 0.125).astype(BF16)
    return first, second


def attend_block(q, keys, values, key_ok):
    outs = []
    for row in head_rows():
        scores = lax.dot_general(
            q * row, keys, (((1,), (1,)), ((), ())), preferred_element_type=F32
        )
        if key_ok is not None:
            scores = jnp.where(key_ok, scores, -1e30)
        highest = jnp.max(scores, axis=-1, keepdims=True)
        weights = jnp.exp(scores - highest)
        total = jnp.sum(weights, axis=-1, keepdims=True)
        outs.append(dot(weights.astype(BF16), values) / total)
    lane = lax.broadcasted_iota(jnp.int32, outs[0].shape, 1)
    return jnp.where(lane < 64, outs[0], outs[1]).astype(BF16)


def window_places(meta):
    core = meta[1] % 2
    return 0, 2, 4, 3 - 2 * core, 1 + 2 * core


def enc_kernel(meta, listed, counts, q, a0, a1, a2, a3, a4, o_out, kept):
    blocks_each = a0.shape[0] // BLOCK
    places = window_places(meta)
    for slot in range(8):
        place = meta[ENC0 + slot]
        which = place // blocks_each
        start = pl.multiple_of((place % blocks_each) * BLOCK, BLOCK)
        for w, array in zip(places, (a0, a1, a2, a3, a4)):

            @pl.when(which == w)
            def _():
                kept[slot] = array[pl.ds(start, BLOCK), :]

    lane = lax.broadcasted_iota(jnp.int32, (1, BLOCK), 1)
    for b in range(2):
        key_ok = jnp.concatenate(
            [lane < counts[listed[b, j]] for j in range(4)], axis=1
        )
        kv = kept[b * 4 : b * 4 + 4].reshape(4 * BLOCK, 256)
        o = attend_block(q[b * BLOCK : (b + 1) * BLOCK, :], kv[:, :128], kv[:, 128:], key_ok)
        for j in range(MP):
            o_out[j, b * BLOCK : (b + 1) * BLOCK, :] = o


def enc_attend(meta, listed, counts, q, windows):
    return pl.pallas_call(
        enc_kernel,
        in_specs=[smem(), smem(), smem()] + [vmem()] * 6,
        out_specs=vmem(),
        out_shape=pltpu.HBM((MP,) + q.shape, BF16),
        scratch_shapes=[pltpu.VMEM((8, BLOCK, 256), BF16)],
        compiler_params=PARAMS,
        name="enc_attend",
    )(meta, listed, counts, q, *windows)


def near_kernel(first_entry, per_block, meta, q, a0, a1, a2, a3, a4, o_out, kept):
    for w, array in zip(window_places(meta), (a0, a1, a2, a3, a4)):
        kept[2 * w] = array[0:BLOCK, :]
        kept[2 * w + 1] = array[BLOCK : 2 * BLOCK, :]
    for b in range(q.shape[0] // BLOCK):
        kv = jnp.concatenate(
            [kept[meta[first_entry + b * per_block + j]] for j in range(per_block)], axis=0
        )
        o = attend_block(q[b * BLOCK : (b + 1) * BLOCK, :], kv[:, :128], kv[:, 128:], None)
        for j in range(MP):
            o_out[j, b * BLOCK : (b + 1) * BLOCK, :] = o


def near_attend(first_entry, per_block, meta, q, windows):
    def body(*refs):
        near_kernel(first_entry, per_block, *refs)

    return pl.pallas_call(
        body,
        in_specs=[smem()] + [vmem()] * 6,
        out_specs=vmem(),
        out_shape=jax.ShapeDtypeStruct((MP,) + q.shape, BF16),
        scratch_shapes=[pltpu.VMEM((10, BLOCK, 256), BF16)],
        compiler_params=PARAMS,
        name="near_attend",
    )(meta, q, *windows)


def prepare_kernel(index, meta, w_own, a1, a2, a3, other, *rest):
    weights = rest[:-4]
    w_out, w_next, w_sems, sems = rest[-4:]
    core = meta[1] % 2
    copies = [
        pltpu.make_async_copy(
            w_own.at[index, :, g * 256 : (g + 1) * 256], w_out.at[g, 0:BLOCK, :], w_sems.at[g, 0]
        )
        for g in range(MP)
    ]
    for part in range(2):
        at = index + 3 * part
        for k, a in enumerate((a1, a2, a3)):
            rows = w_out.at[2 * core + part, (k + 1) * BLOCK : (k + 2) * BLOCK, :]
            copies.append(pltpu.make_async_copy(a.at[2 + at], rows, w_sems.at[part, k + 1]))
            rows = w_out.at[2 * (1 - core) + part, (k + 1) * BLOCK : (k + 2) * BLOCK, :]
            copies.append(pltpu.make_async_copy(other.at[k, at], rows, w_sems.at[2 + part, k + 1]))
    for i, w in enumerate(weights):
        copies.append(
            pltpu.make_async_copy(w.at[index + 1], w_next.at[:, i * 128 : (i + 1) * 128], sems.at[i])
        )
    for copy in copies:
        copy.start()
    for copy in copies:
        copy.wait()


def prepare(index, meta, w_own, fetched, other, weights):
    def body(*refs):
        prepare_kernel(index, *refs)

    operands = (w_own, *fetched, other, *weights)
    return pl.pallas_call(
        body,
        in_specs=[smem()] + [pl.BlockSpec(memory_space=pl.ANY)] * len(operands),
        out_specs=[vmem(), vmem()],
        out_shape=[
            jax.ShapeDtypeStruct((MP, 4 * BLOCK, 256), BF16),
            jax.ShapeDtypeStruct((1024, 128 * len(weights)), BF16),
        ],
        scratch_shapes=[pltpu.SemaphoreType.DMA((MP, MP)), pltpu.SemaphoreType.DMA((3,))],
        compiler_params=PARAMS,
        name="layer_weights",
    )(meta, *operands)


def finish_layer(gain_row, gains, new, w_next):
    rows = normed([new[g] for g in range(MP)])
    row = jnp.concatenate(
        [(rows[g] * gains[gain_row, g : g + 1, :]).astype(BF16) for g in range(MP)], axis=1
    )
    return dot(row, w_next()).astype(BF16)


def first_layer_kernel(meta, o, state, gains, w_own, a1, a2, a3, other, w_k, w_v, w_q, *rest):
    new, kv_out, q_out, kept, sems = rest
    copies = copies_of([(w_k, 1), (w_v, 1), (w_q, 1)], kept, sems)
    for copy in copies:
        copy.start()
    heads = jnp.concatenate([o[source(meta, k)] for k in range(MP)], axis=1)
    new[meta[0]] = state[...]
    for k, a in enumerate((a1, a2, a3)):
        new[source(meta, k + 1)] = a[0:2].reshape(2 * BLOCK, 256)
    core = meta[1] % 2
    for part in range(4):
        at = 3 * (part % 2)
        if part < 2:
            g = 2 * core + part
            fetched = [a[2 + at] for a in (a1, a2, a3)]
        else:
            g = 2 * (1 - core) + part - 2
            fetched = [other[k, at] for k in range(MP - 1)]
        own = w_own[0, :, pl.ds(pl.multiple_of(g * 256, 256), 256)]
        new[g] = (new[g].astype(F32) + dot(heads, jnp.concatenate([own] + fetched, axis=0))).astype(BF16)

    def w_next():
        for copy in copies:
            copy.wait()
        return jnp.concatenate([kept[i] for i in range(3)], axis=1)

    result = finish_layer(2, gains, new, w_next)
    kv_out[...] = result[:, :256]
    q_out[...] = result[:, 256:]


def first_layer(meta, o, state, gains, w_own, fetched, other, weights):
    rows = o.shape[1]
    return pl.pallas_call(
        first_layer_kernel,
        in_specs=[smem()] + [vmem()] * 8 + [hbm()] * 3,
        out_specs=[vmem()] * 3,
        out_shape=[
            jax.ShapeDtypeStruct((MP, rows, 256), BF16),
            jax.ShapeDtypeStruct((rows, 256), BF16),
            jax.ShapeDtypeStruct((rows, 128), BF16),
        ],
        scratch_shapes=[pltpu.VMEM((3, 1024, 128), BF16), pltpu.SemaphoreType.DMA((3,))],
        compiler_params=PARAMS,
        name="first_layer",
    )(meta, o, state, gains, w_own, *fetched, other, *weights)


def layer_kernel(gain_row, meta, o, state, gains, w_out, w_next, *rest):
    last = gain_row == 5
    state_out, kv_out, new = rest[0], rest[1], rest[-1]
    heads = jnp.concatenate([o[source(meta, k)] for k in range(MP)], axis=1)
    for g in range(MP):
        new[g] = (state[g].astype(F32) + dot(heads, w_out[g])).astype(BF16)
        if not last:
            state_out[g] = new[g]
    if last:
        state_out[...] = new[meta[0]]
    result = finish_layer(gain_row, gains, new, lambda: w_next[...])
    kv_out[...] = result[:, :256]
    if not last:
        rest[2][...] = result[:, 256:]


def layer(gain_row, meta, o, state, gains, prepared):
    def body(*refs):
        layer_kernel(gain_row, *refs)

    last = gain_row == 5
    rows = o.shape[1]
    shapes = [
        jax.ShapeDtypeStruct((rows, 256) if last else (MP, rows, 256), BF16),
        jax.ShapeDtypeStruct((rows, 256), BF16),
    ]
    if not last:
        shapes.append(jax.ShapeDtypeStruct((rows, 128), BF16))
    return pl.pallas_call(
        body,
        in_specs=[smem()] + [vmem()] * 5,
        out_specs=[vmem()] * len(shapes),
        out_shape=shapes,
        scratch_shapes=[pltpu.VMEM((MP, rows, 256), BF16)],
        compiler_params=PARAMS,
        name="mesh_layer",
    )(meta, o, state, gains, *prepared)


def final_kernel(meta, counts, o, w_out, grid_in, out):
    tile = grid_in.shape[0]
    heads = jnp.concatenate([o[source(meta, k)] for k in range(MP)], axis=1)
    value = grid_in[...].astype(F32) + dot(heads, w_out[...])
    row = lax.broadcasted_iota(jnp.int32, (BLOCK, 256), 0)
    for b in range(tile // BLOCK):
        count = counts[meta[1] * 8 + pl.program_id(0) * (tile // BLOCK) + b]
        part = value[b * BLOCK : (b + 1) * BLOCK, :]
        out[b * BLOCK : (b + 1) * BLOCK, :] = jnp.where(row < count, part, 0.0).astype(BF16)


def final(meta, counts, o, w_out, grid_in):
    rows = grid_in.shape[0]
    tile = 512
    return pl.pallas_call(
        final_kernel,
        grid=(rows // tile,),
        in_specs=[
            smem(),
            smem(),
            pl.BlockSpec((MP, tile, 128), lambda i: (0, i, 0)),
            vmem(),
            pl.BlockSpec((tile, 256), lambda i: (i, 0)),
        ],
        out_specs=pl.BlockSpec((tile, 256), lambda i: (i, 0)),
        out_shape=jax.ShapeDtypeStruct((rows, 256), BF16),
        compiler_params=PARAMS,
        name="grid_final",
    )(meta, counts, o, w_out, grid_in)


def gather_heads(copies):
    return lax.all_to_all(copies, "mp", split_axis=0, concat_axis=0, tiled=True)


def program(
    grid_in, mesh_in, w_query, w_key, w_value, w_out, norm_gains,
    enc_list, proc_list, dec_list, grid_count,
):
    own_mp, own_node = lax.axis_index("mp"), lax.axis_index("nodes")
    core = own_node % 2
    meta = jnp.concatenate([
        own_mp[None].astype(jnp.int32),
        own_node[None].astype(jnp.int32),
        enc_list.reshape(-1) - (own_node - REACH) * 8,
        proc_list.reshape(-1) - (own_node - REACH) * 2,
        dec_list.reshape(-1) - (own_node - REACH) * 2,
    ])
    gains = norm_gains.reshape(6, MP, 256)
    w_query, w_key, w_value = (
        pltpu.with_memory_space_constraint(w, pltpu.HBM) for w in (w_query, w_key, w_value)
    )

    def gathered(part, name):
        pieces = [part, None, None, None]
        for k in (1, 3, 2):
            pieces[k] = shift_mp(part if name != "w" else part[k], k)
        return pieces

    def window(part):
        low = from_node(part, -2)
        high = from_node(part, 2)
        beside = swap_cores(part)
        beyond = swap_cores(jnp.where(core == 0, high, low))
        return [low, part, high, beside, beyond]

    grid_pieces = gathered(grid_in, "g")
    grid_pieces[0] = pltpu.with_memory_space_constraint(grid_in, pltpu.HBM)

    halves = [lax.dynamic_slice_in_dim(w_out[:3], core * 512 + part * 256, 256, axis=2) for part in range(2)]
    sent = [None] * MP
    for k in (1, 2, 3):
        last = lax.dynamic_slice_in_dim(w_out[3:], (own_mp + k) % MP * 256, 256, axis=2)
        sent[k] = jnp.concatenate([mesh_in.reshape(2, BLOCK, 256)] + halves + [last], axis=0)
    sent[0] = sent[1]
    arrived = gathered(sent, "w")[1:]

    kv = grid_project(1, 0, meta, grid_pieces, gains, w_key, w_value)
    grid_windows = window(kv)
    grid_q = grid_project(4, 3, meta, grid_pieces, gains, w_query)
    w_own = pltpu.with_memory_space_constraint(w_out, pltpu.HBM)
    mesh_q = mesh_start(meta, mesh_in, arrived, gains, w_query)
    o = enc_attend(meta, enc_list, grid_count, mesh_q, grid_windows)

    arrived = lax.optimization_barrier((*arrived, o))[:3]
    other = swap_cores(jnp.stack([a[2:8] for a in arrived]))
    w_last = jnp.concatenate(
        [lax.dynamic_slice_in_dim(w_out[3:], own_mp * 256, 256, axis=2)] + [a[8:] for a in arrived], axis=0
    ).reshape(512, 256)

    state = mesh_in
    for index in range(3):
        heads = gather_heads(o)
        if index == 0:
            made = first_layer(meta, heads, state, gains, w_out, arrived, other, (w_key, w_value, w_query))
        else:
            made = layer(3 if index == 1 else 5, meta, heads, state, gains, prepared)
        state, kv = made[0], made[1]
        near = window(kv)
        if index < 2:
            weights = (w_key, w_value, w_query) if index == 0 else (w_key, w_value)
            prepared = prepare(index + 1, meta, w_own, arrived, other, weights)
            o = near_attend(PROC0, 3, meta, made[2], near)
    o = near_attend(DEC0, 2, meta, grid_q, near)
    heads = gather_heads(o)
    grid_out = final(meta, grid_count, heads, w_last, grid_in)
    return grid_out, state


def solution(mesh):
    placed = (
        P("nodes", "mp"),
        P("nodes", "mp"),
        P(None, None, "mp"),
        P(None, None, "mp"),
        P(None, None, "mp"),
        P(None, "mp", None),
        P(),
        P("nodes", None),
        P("nodes", None),
        P("nodes", None),
        P(),
    )
    return jax.shard_map(
        program,
        mesh=mesh,
        in_specs=placed,
        out_specs=(P("nodes", "mp"), P("nodes", "mp")),
        check_vma=False,
    )
```

```python
import jax
import jax.numpy as jnp
from jax import lax
from jax.experimental import pallas as pl
from jax.experimental.pallas import tpu as pltpu
from jax.sharding import PartitionSpec as P


BLOCK = 128
REACH = 2
EPS = 1e-05
MP = 4
F32 = jnp.float32
BF16 = jnp.bfloat16

ENC0, PROC0, DEC0 = 2, 10, 16


PARAMS = pltpu.CompilerParams(vmem_limit_bytes=16 * 1024 * 1024)


def shift_mp(value, steps):
    return lax.ppermute(value, "mp", [(s, (s + steps) % MP) for s in range(MP)])


def from_node(value, offset):
    count = lax.axis_size("nodes")
    pairs = [(s, s - offset) for s in range(count) if 0 <= s - offset < count]
    return lax.ppermute(value, "nodes", pairs)


def swap_cores(value):
    count = lax.axis_size("nodes")
    return lax.ppermute(value, "nodes", [(s, s ^ 1) for s in range(count)])


def smem():
    return pl.BlockSpec(memory_space=pltpu.SMEM)


def vmem():
    return pl.BlockSpec(memory_space=pltpu.VMEM)


def hbm():
    return pl.BlockSpec(memory_space=pltpu.HBM)


def copies_of(pairs, kept, sems):
    return [
        pltpu.make_async_copy(w.at[layer_index], kept.at[i], sems.at[i])
        for i, (w, layer_index) in enumerate(pairs)
    ]


def source(meta, k):
    return (meta[0] + MP - k) % MP


def normed(pieces):
    width = sum(p.shape[-1] for p in pieces)
    values = [p.astype(F32) for p in pieces]
    mean = sum(jnp.sum(v, axis=-1, keepdims=True) for v in values) * (1.0 / width)
    centred = [v - mean for v in values]
    spread = sum(jnp.sum(c * c, axis=-1, keepdims=True) for c in centred) * (1.0 / width)
    scale = lax.rsqrt(spread + EPS)
    return [c * scale for c in centred]


def dot(a, b):
    return jnp.dot(a, b, preferred_element_type=F32)


def grid_kernel(gain_row, count, meta, x0, x1, x2, x3, gains, *rest):
    weights, out = rest[:count], rest[count]
    rows = normed([x[...] for x in (x0, x1, x2, x3)])
    total = None
    for k in range(MP):
        src = source(meta, k)
        at = pl.ds(pl.multiple_of(src * 256, 256), 256)
        row = (rows[k] * gains[gain_row, pl.ds(src, 1), :]).astype(BF16)
        part = dot(row, jnp.concatenate([w[at, :] for w in weights], axis=1))
        total = part if total is None else total + part
    out[...] = total.astype(BF16)


def grid_project(gain_row, meta, pieces, gains, *weights):
    count = len(weights)

    def body(*refs):
        grid_kernel(gain_row, count, *refs)

    rows = pieces[0].shape[0]
    tile = 256
    return pl.pallas_call(
        body,
        grid=(rows // tile,),
        in_specs=[smem()]
        + [pl.BlockSpec((tile, 256), lambda i: (i, 0))] * MP
        + [vmem()] * (1 + count),
        out_specs=pl.BlockSpec((tile, 128 * count), lambda i: (i, 0)),
        out_shape=jax.ShapeDtypeStruct((rows, 128 * count), BF16),
        cost_estimate=pl.CostEstimate(flops=rows * 1024 * 128 * count * 2, transcendentals=0, bytes_accessed=rows * 4096),
        compiler_params=PARAMS,
        name="grid_project",
    )(meta, *pieces, gains, *weights)


def grid_query_kernel(gain_row, count, layer_index, meta, x0, x1, x2, x3, gains, *rest):
    weights, (out, kept, sems) = rest[:count], rest[count:]
    copies = copies_of([(w, layer_index) for w in weights], kept, sems)

    @pl.when(pl.program_id(0) == 0)
    def _():
        for copy in copies:
            copy.start()

    rows = normed([x[...] for x in (x0, x1, x2, x3)])

    @pl.when(pl.program_id(0) == 0)
    def _():
        for copy in copies:
            copy.wait()

    total = None
    for k in range(MP):
        src = source(meta, k)
        at = pl.ds(pl.multiple_of(src * 256, 256), 256)
        row = (rows[k] * gains[gain_row, pl.ds(src, 1), :]).astype(BF16)
        part = dot(row, jnp.concatenate([kept[i, at, :] for i in range(count)], axis=1))
        total = part if total is None else total + part
    out[...] = total.astype(BF16)


def grid_query(gain_row, layer_index, meta, pieces, gains, *weights):
    count = len(weights)

    def body(*refs):
        grid_query_kernel(gain_row, count, layer_index, *refs)

    rows = pieces[0].shape[0]
    tile = 256
    return pl.pallas_call(
        body,
        grid=(rows // tile,),
        in_specs=[smem()]
        + [pl.BlockSpec((tile, 256), lambda i: (i, 0))] * MP
        + [vmem()]
        + [hbm()] * count,
        out_specs=pl.BlockSpec((tile, 128 * count), lambda i: (i, 0)),
        out_shape=jax.ShapeDtypeStruct((rows, 128 * count), BF16),
        scratch_shapes=[pltpu.VMEM((count, 1024, 128), BF16), pltpu.SemaphoreType.DMA((count,))],
        cost_estimate=pl.CostEstimate(flops=rows * 1024 * 128 * count * 2, transcendentals=0, bytes_accessed=rows * 4096),
        compiler_params=PARAMS,
        name="grid_query",
    )(meta, *pieces, gains, *weights)


def mesh_kernel(meta, x0, a1, a2, a3, gains, w_q, q_out, kept, sems):
    copies = copies_of([(w_q, 0)], kept, sems)
    copies[0].start()
    rows = normed([x0[...]] + [a[...].reshape(2 * BLOCK, 256) for a in (a1, a2, a3)])
    copies[0].wait()
    q = None
    for k in range(MP):
        src = source(meta, k)
        at = pl.ds(pl.multiple_of(src * 256, 256), 256)
        part = dot((rows[k] * gains[0, pl.ds(src, 1), :]).astype(BF16), kept[0, at, :])
        q = part if q is None else q + part
    q_out[...] = q.astype(BF16)


def mesh_start(meta, mesh_in, arrived, gains, w_q):
    rows = mesh_in.shape[0]
    return pl.pallas_call(
        mesh_kernel,
        grid=(1,),
        in_specs=[smem(), vmem()]
        + [pl.BlockSpec((2, BLOCK, 256), lambda i: (0, 0, 0))] * 3
        + [vmem(), hbm()],
        out_specs=vmem(),
        out_shape=jax.ShapeDtypeStruct((rows, 128), BF16),
        scratch_shapes=[pltpu.VMEM((1, 1024, 128), BF16), pltpu.SemaphoreType.DMA((1,))],
        cost_estimate=pl.CostEstimate(flops=rows * 1024 * 128 * 2, transcendentals=0, bytes_accessed=rows * 4096),
        compiler_params=PARAMS,
        name="mesh_start",
    )(meta, mesh_in, *arrived, gains, w_q)


def head_rows():
    lane = lax.broadcasted_iota(jnp.int32, (1, 128), 1)
    first = jnp.where(lane < 64, 0.125, 0.0).astype(BF16)
    second = jnp.where(lane < 64, 0.0, 0.125).astype(BF16)
    return first, second


def attend_block(q, keys, values, key_ok):
    outs = []
    for row in head_rows():
        scores = lax.dot_general(
            q * row, keys, (((1,), (1,)), ((), ())), preferred_element_type=F32
        )
        if key_ok is not None:
            scores = jnp.where(key_ok, scores, -1e30)
        highest = jnp.max(scores, axis=-1, keepdims=True)
        weights = jnp.exp(scores - highest)
        total = jnp.sum(weights, axis=-1, keepdims=True)
        outs.append(dot(weights.astype(BF16), values) / total)
    lane = lax.broadcasted_iota(jnp.int32, outs[0].shape, 1)
    return jnp.where(lane < 64, outs[0], outs[1]).astype(BF16)


def window_places(meta):
    core = meta[1] % 2
    return 0, 2, 4, 3 - 2 * core, 1 + 2 * core


def enc_kernel(meta, listed, counts, q, a0, a1, a2, a3, a4, o_out, kept):
    blocks_each = a0.shape[0] // BLOCK
    places = window_places(meta)
    for slot in range(8):
        place = meta[ENC0 + slot]
        which = place // blocks_each
        start = pl.multiple_of((place % blocks_each) * BLOCK, BLOCK)
        for w, array in zip(places, (a0, a1, a2, a3, a4)):

            @pl.when(which == w)
            def _():
                kept[slot] = array[pl.ds(start, BLOCK), :]

    lane = lax.broadcasted_iota(jnp.int32, (1, BLOCK), 1)
    for b in range(2):
        key_ok = jnp.concatenate(
            [lane < counts[listed[b, j]] for j in range(4)], axis=1
        )
        kv = kept[b * 4 : b * 4 + 4].reshape(4 * BLOCK, 256)
        o = attend_block(q[b * BLOCK : (b + 1) * BLOCK, :], kv[:, :128], kv[:, 128:], key_ok)
        for j in range(MP):
            o_out[j, b * BLOCK : (b + 1) * BLOCK, :] = o


def enc_attend(meta, listed, counts, q, windows):
    return pl.pallas_call(
        enc_kernel,
        in_specs=[smem(), smem(), smem()] + [vmem()] * 6,
        out_specs=vmem(),
        out_shape=pltpu.HBM((MP,) + q.shape, BF16),
        scratch_shapes=[pltpu.VMEM((8, BLOCK, 256), BF16)],
        compiler_params=PARAMS,
        name="enc_attend",
    )(meta, listed, counts, q, *windows)


def near_kernel(first_entry, per_block, meta, q, a0, a1, a2, a3, a4, o_out, kept):
    for w, array in zip(window_places(meta), (a0, a1, a2, a3, a4)):
        kept[2 * w] = array[0:BLOCK, :]
        kept[2 * w + 1] = array[BLOCK : 2 * BLOCK, :]
    for b in range(q.shape[0] // BLOCK):
        kv = jnp.concatenate(
            [kept[meta[first_entry + b * per_block + j]] for j in range(per_block)], axis=0
        )
        o = attend_block(q[b * BLOCK : (b + 1) * BLOCK, :], kv[:, :128], kv[:, 128:], None)
        for j in range(MP):
            o_out[j, b * BLOCK : (b + 1) * BLOCK, :] = o


def near_attend(first_entry, per_block, meta, q, windows):
    def body(*refs):
        near_kernel(first_entry, per_block, *refs)

    return pl.pallas_call(
        body,
        in_specs=[smem()] + [vmem()] * 6,
        out_specs=vmem(),
        out_shape=jax.ShapeDtypeStruct((MP,) + q.shape, BF16),
        scratch_shapes=[pltpu.VMEM((10, BLOCK, 256), BF16)],
        compiler_params=PARAMS,
        name="near_attend",
    )(meta, q, *windows)


def prepare_kernel(index, meta, w_own, a1, a2, a3, other, *rest):
    weights = rest[:-4]
    w_out, w_next, w_sems, sems = rest[-4:]
    core = meta[1] % 2
    copies = [
        pltpu.make_async_copy(
            w_own.at[index, :, g * 256 : (g + 1) * 256], w_out.at[g, 0:BLOCK, :], w_sems.at[g, 0]
        )
        for g in range(MP)
    ]
    for part in range(2):
        at = index + 3 * part
        for k, a in enumerate((a1, a2, a3)):
            rows = w_out.at[2 * core + part, (k + 1) * BLOCK : (k + 2) * BLOCK, :]
            copies.append(pltpu.make_async_copy(a.at[2 + at], rows, w_sems.at[part, k + 1]))
            rows = w_out.at[2 * (1 - core) + part, (k + 1) * BLOCK : (k + 2) * BLOCK, :]
            copies.append(pltpu.make_async_copy(other.at[k, at], rows, w_sems.at[2 + part, k + 1]))
    for i, w in enumerate(weights):
        copies.append(
            pltpu.make_async_copy(w.at[index + 1], w_next.at[:, i * 128 : (i + 1) * 128], sems.at[i])
        )
    for copy in copies:
        copy.start()
    for copy in copies:
        copy.wait()


def prepare(index, meta, w_own, fetched, other, weights):
    def body(*refs):
        prepare_kernel(index, *refs)

    operands = (w_own, *fetched, other, *weights)
    return pl.pallas_call(
        body,
        in_specs=[smem()] + [pl.BlockSpec(memory_space=pl.ANY)] * len(operands),
        out_specs=[vmem(), vmem()],
        out_shape=[
            jax.ShapeDtypeStruct((MP, 4 * BLOCK, 256), BF16),
            jax.ShapeDtypeStruct((1024, 128 * len(weights)), BF16),
        ],
        scratch_shapes=[pltpu.SemaphoreType.DMA((MP, MP)), pltpu.SemaphoreType.DMA((3,))],
        compiler_params=PARAMS,
        name="layer_weights",
    )(meta, *operands)


def finish_layer(gain_row, gains, new, w_next):
    rows = normed([new[g] for g in range(MP)])
    row = jnp.concatenate(
        [(rows[g] * gains[gain_row, g : g + 1, :]).astype(BF16) for g in range(MP)], axis=1
    )
    return dot(row, w_next()).astype(BF16)


def first_layer_kernel(meta, o, state, gains, w_own, a1, a2, a3, other, w_k, w_v, w_q, *rest):
    new, kv_out, q_out, kept, sems = rest
    copies = copies_of([(w_k, 1), (w_v, 1), (w_q, 1)], kept, sems)
    for copy in copies:
        copy.start()
    heads = jnp.concatenate([o[source(meta, k)] for k in range(MP)], axis=1)
    new[meta[0]] = state[...]
    for k, a in enumerate((a1, a2, a3)):
        new[source(meta, k + 1)] = a[0:2].reshape(2 * BLOCK, 256)
    core = meta[1] % 2
    for part in range(4):
        at = 3 * (part % 2)
        if part < 2:
            g = 2 * core + part
            fetched = [a[2 + at] for a in (a1, a2, a3)]
        else:
            g = 2 * (1 - core) + part - 2
            fetched = [other[k, at] for k in range(MP - 1)]
        own = w_own[0, :, pl.ds(pl.multiple_of(g * 256, 256), 256)]
        new[g] = (new[g].astype(F32) + dot(heads, jnp.concatenate([own] + fetched, axis=0))).astype(BF16)

    def w_next():
        for copy in copies:
            copy.wait()
        return jnp.concatenate([kept[i] for i in range(3)], axis=1)

    result = finish_layer(2, gains, new, w_next)
    kv_out[...] = result[:, :256]
    q_out[...] = result[:, 256:]


def first_layer(meta, o, state, gains, w_own, fetched, other, weights):
    rows = o.shape[1]
    return pl.pallas_call(
        first_layer_kernel,
        in_specs=[smem()] + [vmem()] * 8 + [hbm()] * 3,
        out_specs=[vmem()] * 3,
        out_shape=[
            jax.ShapeDtypeStruct((MP, rows, 256), BF16),
            jax.ShapeDtypeStruct((rows, 256), BF16),
            jax.ShapeDtypeStruct((rows, 128), BF16),
        ],
        scratch_shapes=[pltpu.VMEM((3, 1024, 128), BF16), pltpu.SemaphoreType.DMA((3,))],
        compiler_params=PARAMS,
        name="first_layer",
    )(meta, o, state, gains, w_own, *fetched, other, *weights)


def layer_kernel(gain_row, meta, o, state, gains, w_out, w_next, *rest):
    last = gain_row == 5
    state_out, kv_out, new = rest[0], rest[1], rest[-1]
    heads = jnp.concatenate([o[source(meta, k)] for k in range(MP)], axis=1)
    for g in range(MP):
        new[g] = (state[g].astype(F32) + dot(heads, w_out[g])).astype(BF16)
        if not last:
            state_out[g] = new[g]
    if last:
        state_out[...] = new[meta[0]]
    result = finish_layer(gain_row, gains, new, lambda: w_next[...])
    kv_out[...] = result[:, :256]
    if not last:
        rest[2][...] = result[:, 256:]


def layer(gain_row, meta, o, state, gains, prepared):
    def body(*refs):
        layer_kernel(gain_row, *refs)

    last = gain_row == 5
    rows = o.shape[1]
    shapes = [
        jax.ShapeDtypeStruct((rows, 256) if last else (MP, rows, 256), BF16),
        jax.ShapeDtypeStruct((rows, 256), BF16),
    ]
    if not last:
        shapes.append(jax.ShapeDtypeStruct((rows, 128), BF16))
    return pl.pallas_call(
        body,
        in_specs=[smem()] + [vmem()] * 5,
        out_specs=[vmem()] * len(shapes),
        out_shape=shapes,
        scratch_shapes=[pltpu.VMEM((MP, rows, 256), BF16)],
        compiler_params=PARAMS,
        name="mesh_layer",
    )(meta, o, state, gains, *prepared)


def final_kernel(meta, counts, o, w_out, grid_in, out):
    tile = grid_in.shape[0]
    heads = jnp.concatenate([o[source(meta, k)] for k in range(MP)], axis=1)
    value = grid_in[...].astype(F32) + dot(heads, w_out[...])
    row = lax.broadcasted_iota(jnp.int32, (BLOCK, 256), 0)
    for b in range(tile // BLOCK):
        count = counts[meta[1] * 8 + pl.program_id(0) * (tile // BLOCK) + b]
        part = value[b * BLOCK : (b + 1) * BLOCK, :]
        out[b * BLOCK : (b + 1) * BLOCK, :] = jnp.where(row < count, part, 0.0).astype(BF16)


def final(meta, counts, o, w_out, grid_in):
    rows = grid_in.shape[0]
    tile = 512
    return pl.pallas_call(
        final_kernel,
        grid=(rows // tile,),
        in_specs=[
            smem(),
            smem(),
            pl.BlockSpec((MP, tile, 128), lambda i: (0, i, 0)),
            vmem(),
            pl.BlockSpec((tile, 256), lambda i: (i, 0)),
        ],
        out_specs=pl.BlockSpec((tile, 256), lambda i: (i, 0)),
        out_shape=jax.ShapeDtypeStruct((rows, 256), BF16),
        compiler_params=PARAMS,
        name="grid_final",
    )(meta, counts, o, w_out, grid_in)


def gather_heads(copies):
    return lax.all_to_all(copies, "mp", split_axis=0, concat_axis=0, tiled=True)


def program(
    grid_in, mesh_in, w_query, w_key, w_value, w_out, norm_gains,
    enc_list, proc_list, dec_list, grid_count,
):
    own_mp, own_node = lax.axis_index("mp"), lax.axis_index("nodes")
    core = own_node % 2
    meta = jnp.concatenate([
        own_mp[None].astype(jnp.int32),
        own_node[None].astype(jnp.int32),
        enc_list.reshape(-1) - (own_node - REACH) * 8,
        proc_list.reshape(-1) - (own_node - REACH) * 2,
        dec_list.reshape(-1) - (own_node - REACH) * 2,
    ])
    gains = norm_gains.reshape(6, MP, 256)
    w_first = (w_key[0], w_value[0])
    w_query, w_key, w_value = (
        pltpu.with_memory_space_constraint(w, pltpu.HBM) for w in (w_query, w_key, w_value)
    )

    def gathered(part, name):
        pieces = [part, None, None, None]
        for k in (1, 3, 2):
            pieces[k] = shift_mp(part if name != "w" else part[k], k)
        return pieces

    def window(part):
        low = from_node(part, -2)
        high = from_node(part, 2)
        beside = swap_cores(part)
        beyond = swap_cores(jnp.where(core == 0, high, low))
        return [low, part, high, beside, beyond]

    grid_pieces = gathered(grid_in, "g")
    grid_pieces[0] = pltpu.with_memory_space_constraint(grid_in, pltpu.HBM)

    halves = [lax.dynamic_slice_in_dim(w_out[:3], core * 512 + part * 256, 256, axis=2) for part in range(2)]
    sent = [None] * MP
    for k in (1, 2, 3):
        last = lax.dynamic_slice_in_dim(w_out[3:], (own_mp + k) % MP * 256, 256, axis=2)
        sent[k] = jnp.concatenate([mesh_in.reshape(2, BLOCK, 256)] + halves + [last], axis=0)
    sent[0] = sent[1]
    arrived = gathered(sent, "w")[1:]

    kv = grid_project(1, meta, grid_pieces, gains, *w_first)
    grid_windows = window(kv)
    grid_q = grid_query(4, 3, meta, grid_pieces, gains, w_query)
    w_own = pltpu.with_memory_space_constraint(w_out, pltpu.HBM)
    mesh_q = mesh_start(meta, mesh_in, arrived, gains, w_query)
    o = enc_attend(meta, enc_list, grid_count, mesh_q, grid_windows)

    arrived = lax.optimization_barrier((*arrived, o))[:3]
    other = swap_cores(jnp.stack([a[2:8] for a in arrived]))
    w_last = jnp.concatenate(
        [lax.dynamic_slice_in_dim(w_out[3:], own_mp * 256, 256, axis=2)] + [a[8:] for a in arrived], axis=0
    ).reshape(512, 256)

    state = mesh_in
    for index in range(3):
        heads = gather_heads(o)
        if index == 0:
            made = first_layer(meta, heads, state, gains, w_out, arrived, other, (w_key, w_value, w_query))
        else:
            made = layer(3 if index == 1 else 5, meta, heads, state, gains, prepared)
        state, kv = made[0], made[1]
        near = window(kv)
        if index < 2:
            weights = (w_key, w_value, w_query) if index == 0 else (w_key, w_value)
            prepared = prepare(index + 1, meta, w_own, arrived, other, weights)
            o = near_attend(PROC0, 3, meta, made[2], near)
    grid_q, w_last = lax.optimization_barrier((grid_q, w_last))
    o = near_attend(DEC0, 2, meta, grid_q, near)
    heads = gather_heads(o)
    grid_out = final(meta, grid_count, heads, w_last, grid_in)
    return grid_out, state


def solution(mesh):
    placed = (
        P("nodes", "mp"),
        P("nodes", "mp"),
        P(None, None, "mp"),
        P(None, None, "mp"),
        P(None, None, "mp"),
        P(None, "mp", None),
        P(),
        P("nodes", None),
        P("nodes", None),
        P("nodes", None),
        P(),
    )
    return jax.shard_map(
        program,
        mesh=mesh,
        in_specs=placed,
        out_specs=(P("nodes", "mp"), P("nodes", "mp")),
        check_vma=False,
    )
```

```python
import jax
import jax.numpy as jnp
from jax import lax
from jax.experimental import pallas as pl
from jax.experimental.pallas import tpu as pltpu
from jax.sharding import PartitionSpec as P


BLOCK = 128
REACH = 2
EPS = 1e-05
MP = 4
F32 = jnp.float32
BF16 = jnp.bfloat16

ENC0, PROC0, DEC0 = 2, 10, 16


PARAMS = pltpu.CompilerParams(vmem_limit_bytes=16 * 1024 * 1024)


def swap_mp(value, k):
    return lax.ppermute(value, "mp", [(s, s ^ k) for s in range(MP)])


def swap_chips(value, first):
    count = lax.axis_size("nodes") // 2
    pairs = []
    for c in range(first, count - 1, 2):
        for core in range(2):
            pairs += [(2 * c + core, 2 * c + 2 + core), (2 * c + 2 + core, 2 * c + core)]
    return lax.ppermute(value, "nodes", pairs)


def swap_cores(value):
    count = lax.axis_size("nodes")
    return lax.ppermute(value, "nodes", [(s, s ^ 1) for s in range(count)])


def smem():
    return pl.BlockSpec(memory_space=pltpu.SMEM)


def vmem():
    return pl.BlockSpec(memory_space=pltpu.VMEM)


def hbm():
    return pl.BlockSpec(memory_space=pltpu.HBM)


def copies_of(pairs, kept, sems):
    return [
        pltpu.make_async_copy(w.at[layer_index], kept.at[i], sems.at[i])
        for i, (w, layer_index) in enumerate(pairs)
    ]


def source(meta, k):
    return meta[0] ^ k


def normed(pieces):
    width = sum(p.shape[-1] for p in pieces)
    values = [p.astype(F32) for p in pieces]
    mean = sum(jnp.sum(v, axis=-1, keepdims=True) for v in values) * (1.0 / width)
    centred = [v - mean for v in values]
    spread = sum(jnp.sum(c * c, axis=-1, keepdims=True) for c in centred) * (1.0 / width)
    scale = lax.rsqrt(spread + EPS)
    return [c * scale for c in centred]


def dot(a, b):
    return jnp.dot(a, b, preferred_element_type=F32)


def grid_kernel(gain_row, count, meta, x0, x1, x2, x3, gains, *rest):
    weights, out = rest[:count], rest[count]
    rows = normed([x[...] for x in (x0, x1, x2, x3)])
    total = None
    for k in range(MP):
        src = source(meta, k)
        at = pl.ds(pl.multiple_of(src * 256, 256), 256)
        row = (rows[k] * gains[gain_row, pl.ds(src, 1), :]).astype(BF16)
        part = dot(row, jnp.concatenate([w[at, :] for w in weights], axis=1))
        total = part if total is None else total + part
    out[...] = total.astype(BF16)


def grid_project(gain_row, meta, pieces, gains, *weights):
    count = len(weights)

    def body(*refs):
        grid_kernel(gain_row, count, *refs)

    rows = pieces[0].shape[0]
    tile = 256
    return pl.pallas_call(
        body,
        grid=(rows // tile,),
        in_specs=[smem()]
        + [pl.BlockSpec((tile, 256), lambda i: (i, 0))] * MP
        + [vmem()] * (1 + count),
        out_specs=pl.BlockSpec((tile, 128 * count), lambda i: (i, 0)),
        out_shape=jax.ShapeDtypeStruct((rows, 128 * count), BF16),
        cost_estimate=pl.CostEstimate(flops=rows * 1024 * 128 * count * 2, transcendentals=0, bytes_accessed=rows * 4096),
        compiler_params=PARAMS,
        name="grid_project",
    )(meta, *pieces, gains, *weights)


def grid_query_kernel(gain_row, count, layer_index, meta, x0, x1, x2, x3, gains, *rest):
    weights, (out, kept, sems) = rest[:count], rest[count:]
    copies = copies_of([(w, layer_index) for w in weights], kept, sems)

    @pl.when(pl.program_id(0) == 0)
    def _():
        for copy in copies:
            copy.start()

    rows = normed([x[...] for x in (x0, x1, x2, x3)])

    @pl.when(pl.program_id(0) == 0)
    def _():
        for copy in copies:
            copy.wait()

    total = None
    for k in range(MP):
        src = source(meta, k)
        at = pl.ds(pl.multiple_of(src * 256, 256), 256)
        row = (rows[k] * gains[gain_row, pl.ds(src, 1), :]).astype(BF16)
        part = dot(row, jnp.concatenate([kept[i, at, :] for i in range(count)], axis=1))
        total = part if total is None else total + part
    out[...] = total.astype(BF16)


def grid_query(gain_row, layer_index, meta, pieces, gains, *weights):
    count = len(weights)

    def body(*refs):
        grid_query_kernel(gain_row, count, layer_index, *refs)

    rows = pieces[0].shape[0]
    tile = 256
    return pl.pallas_call(
        body,
        grid=(rows // tile,),
        in_specs=[smem()]
        + [pl.BlockSpec((tile, 256), lambda i: (i, 0))] * MP
        + [vmem()]
        + [hbm()] * count,
        out_specs=pl.BlockSpec((tile, 128 * count), lambda i: (i, 0)),
        out_shape=jax.ShapeDtypeStruct((rows, 128 * count), BF16),
        scratch_shapes=[pltpu.VMEM((count, 1024, 128), BF16), pltpu.SemaphoreType.DMA((count,))],
        cost_estimate=pl.CostEstimate(flops=rows * 1024 * 128 * count * 2, transcendentals=0, bytes_accessed=rows * 4096),
        compiler_params=PARAMS,
        name="grid_query",
    )(meta, *pieces, gains, *weights)


def mesh_kernel(meta, x0, a1, a2, a3, gains, w_q, q_out, kept, sems):
    copies = copies_of([(w_q, 0)], kept, sems)
    copies[0].start()
    rows = normed([x0[...]] + [a[...].reshape(2 * BLOCK, 256) for a in (a1, a2, a3)])
    copies[0].wait()
    q = None
    for k in range(MP):
        src = source(meta, k)
        at = pl.ds(pl.multiple_of(src * 256, 256), 256)
        part = dot((rows[k] * gains[0, pl.ds(src, 1), :]).astype(BF16), kept[0, at, :])
        q = part if q is None else q + part
    q_out[...] = q.astype(BF16)


def mesh_start(meta, mesh_in, arrived, gains, w_q):
    rows = mesh_in.shape[0]
    return pl.pallas_call(
        mesh_kernel,
        grid=(1,),
        in_specs=[smem(), vmem()]
        + [pl.BlockSpec((2, BLOCK, 256), lambda i: (0, 0, 0))] * 3
        + [vmem(), hbm()],
        out_specs=vmem(),
        out_shape=jax.ShapeDtypeStruct((rows, 128), BF16),
        scratch_shapes=[pltpu.VMEM((1, 1024, 128), BF16), pltpu.SemaphoreType.DMA((1,))],
        cost_estimate=pl.CostEstimate(flops=rows * 1024 * 128 * 2, transcendentals=0, bytes_accessed=rows * 4096),
        compiler_params=PARAMS,
        name="mesh_start",
    )(meta, mesh_in, *arrived, gains, w_q)


def head_rows():
    lane = lax.broadcasted_iota(jnp.int32, (1, 128), 1)
    first = jnp.where(lane < 64, 0.125, 0.0).astype(BF16)
    second = jnp.where(lane < 64, 0.0, 0.125).astype(BF16)
    return first, second


def attend_block(q, keys, values, key_ok):
    outs = []
    for row in head_rows():
        scores = lax.dot_general(
            q * row, keys, (((1,), (1,)), ((), ())), preferred_element_type=F32
        )
        if key_ok is not None:
            scores = jnp.where(key_ok, scores, -1e30)
        highest = jnp.max(scores, axis=-1, keepdims=True)
        weights = jnp.exp(scores - highest)
        total = jnp.sum(weights, axis=-1, keepdims=True)
        outs.append(dot(weights.astype(BF16), values) / total)
    lane = lax.broadcasted_iota(jnp.int32, outs[0].shape, 1)
    return jnp.where(lane < 64, outs[0], outs[1]).astype(BF16)


def window_places(meta):
    core = meta[1] % 2
    odd = meta[1] // 2 % 2
    return 4 * odd, 2, 4 - 4 * odd, 3 - 2 * core, 1 + 2 * core


def enc_kernel(meta, listed, counts, q, a0, a1, a2, a3, a4, o_out, kept):
    blocks_each = a0.shape[0] // BLOCK
    places = window_places(meta)
    for slot in range(8):
        place = meta[ENC0 + slot]
        which = place // blocks_each
        start = pl.multiple_of((place % blocks_each) * BLOCK, BLOCK)
        for w, array in zip(places, (a0, a1, a2, a3, a4)):

            @pl.when(which == w)
            def _():
                kept[slot] = array[pl.ds(start, BLOCK), :]

    lane = lax.broadcasted_iota(jnp.int32, (1, BLOCK), 1)
    for b in range(2):
        key_ok = jnp.concatenate(
            [lane < counts[listed[b, j]] for j in range(4)], axis=1
        )
        kv = kept[b * 4 : b * 4 + 4].reshape(4 * BLOCK, 256)
        o = attend_block(q[b * BLOCK : (b + 1) * BLOCK, :], kv[:, :128], kv[:, 128:], key_ok)
        for j in range(MP):
            o_out[j, b * BLOCK : (b + 1) * BLOCK, :] = o


def enc_attend(meta, listed, counts, q, windows):
    return pl.pallas_call(
        enc_kernel,
        in_specs=[smem(), smem(), smem()] + [vmem()] * 6,
        out_specs=vmem(),
        out_shape=pltpu.HBM((MP,) + q.shape, BF16),
        scratch_shapes=[pltpu.VMEM((8, BLOCK, 256), BF16)],
        compiler_params=PARAMS,
        name="enc_attend",
    )(meta, listed, counts, q, *windows)


def near_kernel(first_entry, per_block, meta, q, a0, a1, a2, a3, a4, o_out, kept):
    for w, array in zip(window_places(meta), (a0, a1, a2, a3, a4)):
        kept[2 * w] = array[0:BLOCK, :]
        kept[2 * w + 1] = array[BLOCK : 2 * BLOCK, :]
    for b in range(q.shape[0] // BLOCK):
        kv = jnp.concatenate(
            [kept[meta[first_entry + b * per_block + j]] for j in range(per_block)], axis=0
        )
        o = attend_block(q[b * BLOCK : (b + 1) * BLOCK, :], kv[:, :128], kv[:, 128:], None)
        for j in range(MP):
            o_out[j, b * BLOCK : (b + 1) * BLOCK, :] = o


def near_attend(first_entry, per_block, meta, q, windows):
    def body(*refs):
        near_kernel(first_entry, per_block, *refs)

    return pl.pallas_call(
        body,
        in_specs=[smem()] + [vmem()] * 6,
        out_specs=vmem(),
        out_shape=jax.ShapeDtypeStruct((MP,) + q.shape, BF16),
        scratch_shapes=[pltpu.VMEM((10, BLOCK, 256), BF16)],
        compiler_params=PARAMS,
        name="near_attend",
    )(meta, q, *windows)


def prepare_kernel(index, meta, w_own, a1, a2, a3, other, *rest):
    weights = rest[:-4]
    w_out, w_next, w_sems, sems = rest[-4:]
    core = meta[1] % 2
    copies = [
        pltpu.make_async_copy(
            w_own.at[index, :, g * 256 : (g + 1) * 256], w_out.at[g, 0:BLOCK, :], w_sems.at[g, 0]
        )
        for g in range(MP)
    ]
    for part in range(2):
        at = index + 3 * part
        for k, a in enumerate((a1, a2, a3)):
            rows = w_out.at[2 * core + part, (k + 1) * BLOCK : (k + 2) * BLOCK, :]
            copies.append(pltpu.make_async_copy(a.at[2 + at], rows, w_sems.at[part, k + 1]))
            rows = w_out.at[2 * (1 - core) + part, (k + 1) * BLOCK : (k + 2) * BLOCK, :]
            copies.append(pltpu.make_async_copy(other.at[k, at], rows, w_sems.at[2 + part, k + 1]))
    for i, w in enumerate(weights):
        copies.append(
            pltpu.make_async_copy(w.at[index + 1], w_next.at[:, i * 128 : (i + 1) * 128], sems.at[i])
        )
    for copy in copies:
        copy.start()
    for copy in copies:
        copy.wait()


def prepare(index, meta, w_own, fetched, other, weights):
    def body(*refs):
        prepare_kernel(index, *refs)

    operands = (w_own, *fetched, other, *weights)
    return pl.pallas_call(
        body,
        in_specs=[smem()] + [pl.BlockSpec(memory_space=pl.ANY)] * len(operands),
        out_specs=[vmem(), vmem()],
        out_shape=[
            jax.ShapeDtypeStruct((MP, 4 * BLOCK, 256), BF16),
            jax.ShapeDtypeStruct((1024, 128 * len(weights)), BF16),
        ],
        scratch_shapes=[pltpu.SemaphoreType.DMA((MP, MP)), pltpu.SemaphoreType.DMA((3,))],
        compiler_params=PARAMS,
        name="layer_weights",
    )(meta, *operands)


def finish_layer(gain_row, gains, new, w_next):
    rows = normed([new[g] for g in range(MP)])
    row = jnp.concatenate(
        [(rows[g] * gains[gain_row, g : g + 1, :]).astype(BF16) for g in range(MP)], axis=1
    )
    return dot(row, w_next()).astype(BF16)


def first_layer_kernel(meta, o, state, gains, w_own, a1, a2, a3, other, w_k, w_v, w_q, *rest):
    new, kv_out, q_out, kept, sems = rest
    copies = copies_of([(w_k, 1), (w_v, 1), (w_q, 1)], kept, sems)
    for copy in copies:
        copy.start()
    heads = jnp.concatenate([o[source(meta, k)] for k in range(MP)], axis=1)
    new[meta[0]] = state[...]
    for k, a in enumerate((a1, a2, a3)):
        new[source(meta, k + 1)] = a[0:2].reshape(2 * BLOCK, 256)
    core = meta[1] % 2
    for part in range(4):
        at = 3 * (part % 2)
        if part < 2:
            g = 2 * core + part
            fetched = [a[2 + at] for a in (a1, a2, a3)]
        else:
            g = 2 * (1 - core) + part - 2
            fetched = [other[k, at] for k in range(MP - 1)]
        own = w_own[0, :, pl.ds(pl.multiple_of(g * 256, 256), 256)]
        new[g] = (new[g].astype(F32) + dot(heads, jnp.concatenate([own] + fetched, axis=0))).astype(BF16)

    def w_next():
        for copy in copies:
            copy.wait()
        return jnp.concatenate([kept[i] for i in range(3)], axis=1)

    result = finish_layer(2, gains, new, w_next)
    kv_out[...] = result[:, :256]
    q_out[...] = result[:, 256:]


def first_layer(meta, o, state, gains, w_own, fetched, other, weights):
    rows = o.shape[1]
    return pl.pallas_call(
        first_layer_kernel,
        in_specs=[smem()] + [vmem()] * 8 + [hbm()] * 3,
        out_specs=[vmem()] * 3,
        out_shape=[
            jax.ShapeDtypeStruct((MP, rows, 256), BF16),
            jax.ShapeDtypeStruct((rows, 256), BF16),
            jax.ShapeDtypeStruct((rows, 128), BF16),
        ],
        scratch_shapes=[pltpu.VMEM((3, 1024, 128), BF16), pltpu.SemaphoreType.DMA((3,))],
        compiler_params=PARAMS,
        name="first_layer",
    )(meta, o, state, gains, w_own, *fetched, other, *weights)


def layer_kernel(gain_row, meta, o, state, gains, w_out, w_next, *rest):
    last = gain_row == 5
    state_out, kv_out, new = rest[0], rest[1], rest[-1]
    heads = jnp.concatenate([o[source(meta, k)] for k in range(MP)], axis=1)
    for g in range(MP):
        new[g] = (state[g].astype(F32) + dot(heads, w_out[g])).astype(BF16)
        if not last:
            state_out[g] = new[g]
    if last:
        state_out[...] = new[meta[0]]
    result = finish_layer(gain_row, gains, new, lambda: w_next[...])
    kv_out[...] = result[:, :256]
    if not last:
        rest[2][...] = result[:, 256:]


def layer(gain_row, meta, o, state, gains, prepared):
    def body(*refs):
        layer_kernel(gain_row, *refs)

    last = gain_row == 5
    rows = o.shape[1]
    shapes = [
        jax.ShapeDtypeStruct((rows, 256) if last else (MP, rows, 256), BF16),
        jax.ShapeDtypeStruct((rows, 256), BF16),
    ]
    if not last:
        shapes.append(jax.ShapeDtypeStruct((rows, 128), BF16))
    return pl.pallas_call(
        body,
        in_specs=[smem()] + [vmem()] * 5,
        out_specs=[vmem()] * len(shapes),
        out_shape=shapes,
        scratch_shapes=[pltpu.VMEM((MP, rows, 256), BF16)],
        compiler_params=PARAMS,
        name="mesh_layer",
    )(meta, o, state, gains, *prepared)


def final_kernel(meta, counts, o, w_out, grid_in, out):
    tile = grid_in.shape[0]
    heads = jnp.concatenate([o[source(meta, k)] for k in range(MP)], axis=1)
    value = grid_in[...].astype(F32) + dot(heads, w_out[...])
    row = lax.broadcasted_iota(jnp.int32, (BLOCK, 256), 0)
    for b in range(tile // BLOCK):
        count = counts[meta[1] * 8 + pl.program_id(0) * (tile // BLOCK) + b]
        part = value[b * BLOCK : (b + 1) * BLOCK, :]
        out[b * BLOCK : (b + 1) * BLOCK, :] = jnp.where(row < count, part, 0.0).astype(BF16)


def final(meta, counts, o, w_out, grid_in):
    rows = grid_in.shape[0]
    tile = 512
    return pl.pallas_call(
        final_kernel,
        grid=(rows // tile,),
        in_specs=[
            smem(),
            smem(),
            pl.BlockSpec((MP, tile, 128), lambda i: (0, i, 0)),
            vmem(),
            pl.BlockSpec((tile, 256), lambda i: (i, 0)),
        ],
        out_specs=pl.BlockSpec((tile, 256), lambda i: (i, 0)),
        out_shape=jax.ShapeDtypeStruct((rows, 256), BF16),
        compiler_params=PARAMS,
        name="grid_final",
    )(meta, counts, o, w_out, grid_in)


def gather_heads(copies):
    return lax.all_to_all(copies, "mp", split_axis=0, concat_axis=0, tiled=True)


def program(
    grid_in, mesh_in, w_query, w_key, w_value, w_out, norm_gains,
    enc_list, proc_list, dec_list, grid_count,
):
    own_mp, own_node = lax.axis_index("mp"), lax.axis_index("nodes")
    core = own_node % 2
    meta = jnp.concatenate([
        own_mp[None].astype(jnp.int32),
        own_node[None].astype(jnp.int32),
        enc_list.reshape(-1) - (own_node - REACH) * 8,
        proc_list.reshape(-1) - (own_node - REACH) * 2,
        dec_list.reshape(-1) - (own_node - REACH) * 2,
    ])
    gains = norm_gains.reshape(6, MP, 256)
    w_first = (w_key[0], w_value[0])
    w_query, w_key, w_value = (
        pltpu.with_memory_space_constraint(w, pltpu.HBM) for w in (w_query, w_key, w_value)
    )

    def gathered(part, name):
        pieces = [part, None, None, None]
        for k in (1, 3, 2):
            pieces[k] = swap_mp(part if name != "w" else part[k], k)
        return pieces

    def window(part):
        across = swap_chips(part, 1)
        within = swap_chips(part, 0)
        beside = swap_cores(part)
        beyond = swap_cores(jnp.where((core == 0) == (own_node // 2 % 2 == 0), within, across))
        return [across, part, within, beside, beyond]

    grid_pieces = gathered(grid_in, "g")
    grid_pieces[0] = pltpu.with_memory_space_constraint(grid_in, pltpu.HBM)

    halves = [lax.dynamic_slice_in_dim(w_out[:3], core * 512 + part * 256, 256, axis=2) for part in range(2)]
    sent = [None] * MP
    for k in (1, 2, 3):
        last = lax.dynamic_slice_in_dim(w_out[3:], (own_mp ^ k) * 256, 256, axis=2)
        sent[k] = jnp.concatenate([mesh_in.reshape(2, BLOCK, 256)] + halves + [last], axis=0)
    sent[0] = sent[1]
    arrived = gathered(sent, "w")[1:]

    kv = grid_project(1, meta, grid_pieces, gains, *w_first)
    grid_windows = window(kv)
    grid_q = grid_query(4, 3, meta, grid_pieces, gains, w_query)
    w_own = pltpu.with_memory_space_constraint(w_out, pltpu.HBM)
    mesh_q = mesh_start(meta, mesh_in, arrived, gains, w_query)
    o = enc_attend(meta, enc_list, grid_count, mesh_q, grid_windows)

    arrived = lax.optimization_barrier((*arrived, o))[:3]
    other = swap_cores(jnp.stack([a[2:8] for a in arrived]))
    w_last = jnp.concatenate(
        [lax.dynamic_slice_in_dim(w_out[3:], own_mp * 256, 256, axis=2)] + [a[8:] for a in arrived], axis=0
    ).reshape(512, 256)

    state = mesh_in
    for index in range(3):
        heads = gather_heads(o)
        if index == 0:
            made = first_layer(meta, heads, state, gains, w_out, arrived, other, (w_key, w_value, w_query))
        else:
            made = layer(3 if index == 1 else 5, meta, heads, state, gains, prepared)
        state, kv = made[0], made[1]
        near = window(kv)
        if index < 2:
            weights = (w_key, w_value, w_query) if index == 0 else (w_key, w_value)
            prepared = prepare(index + 1, meta, w_own, arrived, other, weights)
            o = near_attend(PROC0, 3, meta, made[2], near)
    grid_q, w_last = lax.optimization_barrier((grid_q, w_last))
    o = near_attend(DEC0, 2, meta, grid_q, near)
    heads = gather_heads(o)
    grid_out = final(meta, grid_count, heads, w_last, grid_in)
    return grid_out, state


def solution(mesh):
    placed = (
        P("nodes", "mp"),
        P("nodes", "mp"),
        P(None, None, "mp"),
        P(None, None, "mp"),
        P(None, None, "mp"),
        P(None, "mp", None),
        P(),
        P("nodes", None),
        P("nodes", None),
        P("nodes", None),
        P(),
    )
    return jax.shard_map(
        program,
        mesh=mesh,
        in_specs=placed,
        out_specs=(P("nodes", "mp"), P("nodes", "mp")),
        check_vma=False,
    )
```

```python
import jax
import jax.numpy as jnp
from jax import lax
from jax.experimental import pallas as pl
from jax.experimental.pallas import tpu as pltpu
from jax.sharding import PartitionSpec as P


BLOCK = 128
REACH = 2
EPS = 1e-05
MP = 4
F32 = jnp.float32
BF16 = jnp.bfloat16

ENC0, PROC0, DEC0 = 2, 10, 16


PARAMS = pltpu.CompilerParams(vmem_limit_bytes=16 * 1024 * 1024)


def swap_mp(value, k):
    return lax.ppermute(value, "mp", [(s, s ^ k) for s in range(MP)])


def swap_chips(value, first):
    count = lax.axis_size("nodes") // 2
    pairs = []
    for c in range(first, count - 1, 2):
        for core in range(2):
            pairs += [(2 * c + core, 2 * c + 2 + core), (2 * c + 2 + core, 2 * c + core)]
    return lax.ppermute(value, "nodes", pairs)


def swap_cores(value):
    count = lax.axis_size("nodes")
    return lax.ppermute(value, "nodes", [(s, s ^ 1) for s in range(count)])


def smem():
    return pl.BlockSpec(memory_space=pltpu.SMEM)


def vmem():
    return pl.BlockSpec(memory_space=pltpu.VMEM)


def hbm():
    return pl.BlockSpec(memory_space=pltpu.HBM)


def copies_of(pairs, kept, sems):
    return [
        pltpu.make_async_copy(w.at[layer_index], kept.at[i], sems.at[i])
        for i, (w, layer_index) in enumerate(pairs)
    ]


def source(meta, k):
    return meta[0] ^ k


def normed(pieces):
    width = sum(p.shape[-1] for p in pieces)
    values = [p.astype(F32) for p in pieces]
    mean = sum(jnp.sum(v, axis=-1, keepdims=True) for v in values) * (1.0 / width)
    centred = [v - mean for v in values]
    spread = sum(jnp.sum(c * c, axis=-1, keepdims=True) for c in centred) * (1.0 / width)
    scale = lax.rsqrt(spread + EPS)
    return [c * scale for c in centred]


def dot(a, b):
    return jnp.dot(a, b, preferred_element_type=F32)


def grid_kernel(gain_row, count, layer_index, meta, x0, x1, x2, x3, gains, *rest):
    weights, (out, kept, sems) = rest[:count], rest[count:]
    copies = copies_of([(w, layer_index) for w in weights], kept, sems)

    @pl.when(pl.program_id(0) == 0)
    def _():
        for copy in copies:
            copy.start()

    rows = normed([x[...] for x in (x0, x1, x2, x3)])

    @pl.when(pl.program_id(0) == 0)
    def _():
        for copy in copies:
            copy.wait()

    total = None
    for k in range(MP):
        src = source(meta, k)
        at = pl.ds(pl.multiple_of(src * 256, 256), 256)
        row = (rows[k] * gains[gain_row, pl.ds(src, 1), :]).astype(BF16)
        part = dot(row, jnp.concatenate([kept[i, at, :] for i in range(count)], axis=1))
        total = part if total is None else total + part
    out[...] = total.astype(BF16)


def grid_project(gain_row, layer_index, meta, pieces, gains, *weights):
    count = len(weights)

    def body(*refs):
        grid_kernel(gain_row, count, layer_index, *refs)

    rows = pieces[0].shape[0]
    tile = 256
    return pl.pallas_call(
        body,
        grid=(rows // tile,),
        in_specs=[smem()]
        + [pl.BlockSpec((tile, 256), lambda i: (i, 0))] * MP
        + [vmem()]
        + [hbm()] * count,
        out_specs=pl.BlockSpec((tile, 128 * count), lambda i: (i, 0)),
        out_shape=jax.ShapeDtypeStruct((rows, 128 * count), BF16),
        scratch_shapes=[pltpu.VMEM((count, 1024, 128), BF16), pltpu.SemaphoreType.DMA((count,))],
        cost_estimate=pl.CostEstimate(flops=rows * 1024 * 128 * count * 2, transcendentals=0, bytes_accessed=rows * 4096),
        compiler_params=PARAMS,
        name="grid_project",
    )(meta, *pieces, gains, *weights)


def mesh_kernel(meta, x0, a1, a2, a3, gains, w_q, q_out, kept, sems):
    copies = copies_of([(w_q, 0)], kept, sems)
    copies[0].start()
    rows = normed([x0[...]] + [a[...].reshape(2 * BLOCK, 256) for a in (a1, a2, a3)])
    copies[0].wait()
    q = None
    for k in range(MP):
        src = source(meta, k)
        at = pl.ds(pl.multiple_of(src * 256, 256), 256)
        part = dot((rows[k] * gains[0, pl.ds(src, 1), :]).astype(BF16), kept[0, at, :])
        q = part if q is None else q + part
    q_out[...] = q.astype(BF16)


def mesh_start(meta, mesh_in, arrived, gains, w_q):
    rows = mesh_in.shape[0]
    return pl.pallas_call(
        mesh_kernel,
        grid=(1,),
        in_specs=[smem(), vmem()]
        + [pl.BlockSpec((2, BLOCK, 256), lambda i: (0, 0, 0))] * 3
        + [vmem(), hbm()],
        out_specs=vmem(),
        out_shape=jax.ShapeDtypeStruct((rows, 128), BF16),
        scratch_shapes=[pltpu.VMEM((1, 1024, 128), BF16), pltpu.SemaphoreType.DMA((1,))],
        cost_estimate=pl.CostEstimate(flops=rows * 1024 * 128 * 2, transcendentals=0, bytes_accessed=rows * 4096),
        compiler_params=PARAMS,
        name="mesh_start",
    )(meta, mesh_in, *arrived, gains, w_q)


def head_rows():
    lane = lax.broadcasted_iota(jnp.int32, (1, 128), 1)
    first = jnp.where(lane < 64, 0.125, 0.0).astype(BF16)
    second = jnp.where(lane < 64, 0.0, 0.125).astype(BF16)
    return first, second


def attend_block(q, keys, values, key_ok):
    outs = []
    for row in head_rows():
        scores = lax.dot_general(
            q * row, keys, (((1,), (1,)), ((), ())), preferred_element_type=F32
        )
        if key_ok is not None:
            scores = jnp.where(key_ok, scores, -1e30)
        highest = jnp.max(scores, axis=-1, keepdims=True)
        weights = jnp.exp(scores - highest)
        total = jnp.sum(weights, axis=-1, keepdims=True)
        outs.append(dot(weights.astype(BF16), values) / total)
    lane = lax.broadcasted_iota(jnp.int32, outs[0].shape, 1)
    return jnp.where(lane < 64, outs[0], outs[1]).astype(BF16)


def window_places(meta):
    core = meta[1] % 2
    odd = meta[1] // 2 % 2
    return 4 * odd, 2, 4 - 4 * odd, 3 - 2 * core, 1 + 2 * core


def enc_kernel(meta, listed, counts, q, a0, a1, a2, a3, a4, o_out, kept):
    blocks_each = a0.shape[0] // BLOCK
    places = window_places(meta)
    for slot in range(8):
        place = meta[ENC0 + slot]
        which = place // blocks_each
        start = pl.multiple_of((place % blocks_each) * BLOCK, BLOCK)
        for w, array in zip(places, (a0, a1, a2, a3, a4)):

            @pl.when(which == w)
            def _():
                kept[slot] = array[pl.ds(start, BLOCK), :]

    lane = lax.broadcasted_iota(jnp.int32, (1, BLOCK), 1)
    for b in range(2):
        key_ok = jnp.concatenate(
            [lane < counts[listed[b, j]] for j in range(4)], axis=1
        )
        kv = kept[b * 4 : b * 4 + 4].reshape(4 * BLOCK, 256)
        o = attend_block(q[b * BLOCK : (b + 1) * BLOCK, :], kv[:, :128], kv[:, 128:], key_ok)
        for j in range(MP):
            o_out[j, b * BLOCK : (b + 1) * BLOCK, :] = o


def enc_attend(meta, listed, counts, q, windows):
    return pl.pallas_call(
        enc_kernel,
        in_specs=[smem(), smem(), smem()] + [vmem()] * 6,
        out_specs=vmem(),
        out_shape=pltpu.HBM((MP,) + q.shape, BF16),
        scratch_shapes=[pltpu.VMEM((8, BLOCK, 256), BF16)],
        compiler_params=PARAMS,
        name="enc_attend",
    )(meta, listed, counts, q, *windows)


def near_kernel(first_entry, per_block, meta, q, a0, a1, a2, a3, a4, o_out, kept):
    for w, array in zip(window_places(meta), (a0, a1, a2, a3, a4)):
        kept[2 * w] = array[0:BLOCK, :]
        kept[2 * w + 1] = array[BLOCK : 2 * BLOCK, :]
    for b in range(q.shape[0] // BLOCK):
        kv = jnp.concatenate(
            [kept[meta[first_entry + b * per_block + j]] for j in range(per_block)], axis=0
        )
        o = attend_block(q[b * BLOCK : (b + 1) * BLOCK, :], kv[:, :128], kv[:, 128:], None)
        for j in range(MP):
            o_out[j, b * BLOCK : (b + 1) * BLOCK, :] = o


def near_attend(first_entry, per_block, meta, q, windows):
    def body(*refs):
        near_kernel(first_entry, per_block, *refs)

    return pl.pallas_call(
        body,
        in_specs=[smem()] + [vmem()] * 6,
        out_specs=vmem(),
        out_shape=jax.ShapeDtypeStruct((MP,) + q.shape, BF16),
        scratch_shapes=[pltpu.VMEM((10, BLOCK, 256), BF16)],
        compiler_params=PARAMS,
        name="near_attend",
    )(meta, q, *windows)


def layer_kernel(index, meta, o, state, gains, w_own, lo1, lo2, lo3, hi1, hi2, hi3, other_lo, other_hi, *rest):
    last = index == 2
    mesh, rest = rest[: 3 * (index == 0)], rest[3 * (index == 0) :]
    count = 2 if last else 3
    weights, outs, (kept, sems) = rest[:count], rest[count:-2], rest[-2:]
    new = outs[-1] if last else outs[0]
    copies = copies_of([(w, index + 1) for w in weights], kept, sems)
    for copy in copies:
        copy.start()
    heads = jnp.concatenate([o[source(meta, k)] for k in range(MP)], axis=1)
    if index == 0:
        new[meta[0]] = state[...]
        for k, a in enumerate(mesh):
            new[source(meta, k + 1)] = a[...].reshape(2 * BLOCK, 256)
        state = new
    core = meta[1] % 2
    for part in range(4):
        if part < 2:
            g = 2 * core + part
            fetched = [a[0] for a in ((lo1, lo2, lo3), (hi1, hi2, hi3))[part]]
        else:
            g = 2 * (1 - core) + part - 2
            other = (other_lo, other_hi)[part - 2]
            fetched = [other[k, 0] for k in range(MP - 1)]
        own = w_own[0, :, pl.ds(pl.multiple_of(g * 256, 256), 256)]
        new[g] = (state[g].astype(F32) + dot(heads, jnp.concatenate([own] + fetched, axis=0))).astype(BF16)
    if last:
        outs[0][...] = new[meta[0]]
    rows = normed([new[g] for g in range(MP)])
    gain_row = 5 if last else index + 2
    row = jnp.concatenate(
        [(rows[g] * gains[gain_row, g : g + 1, :]).astype(BF16) for g in range(MP)], axis=1
    )
    for copy in copies:
        copy.wait()
    result = dot(row, jnp.concatenate([kept[i] for i in range(count)], axis=1)).astype(BF16)
    outs[1][...] = result[:, :256]
    if not last:
        outs[2][...] = result[:, 256:]


def layer(index, meta, o, state, gains, w_own, fetched, other, weights):
    def body(*refs):
        layer_kernel(index, *refs)

    def block(at):
        return pl.BlockSpec((1, BLOCK, 256), lambda i: (at, 0, 0))

    def other_block(at):
        return pl.BlockSpec((MP - 1, 1, BLOCK, 256), lambda i: (0, at, 0, 0))

    last = index == 2
    rows = o.shape[1]
    shapes = [
        jax.ShapeDtypeStruct((rows, 256) if last else (MP, rows, 256), BF16),
        jax.ShapeDtypeStruct((rows, 256), BF16),
    ]
    if not last:
        shapes.append(jax.ShapeDtypeStruct((rows, 128), BF16))
    mesh = fetched if index == 0 else ()
    weights = weights[:2] if last else weights
    scratch = [pltpu.VMEM((MP, rows, 256), BF16)] if last else []
    return pl.pallas_call(
        body,
        grid=(1,),
        in_specs=[smem()]
        + [vmem()] * 3
        + [pl.BlockSpec((1, BLOCK, 1024), lambda i: (index, 0, 0))]
        + [block(2 + index)] * 3
        + [block(5 + index)] * 3
        + [other_block(index), other_block(3 + index)]
        + [pl.BlockSpec((2, BLOCK, 256), lambda i: (0, 0, 0))] * len(mesh)
        + [hbm()] * len(weights),
        out_specs=[vmem()] * len(shapes),
        out_shape=shapes,
        scratch_shapes=scratch + [pltpu.VMEM((3, 1024, 128), BF16), pltpu.SemaphoreType.DMA((3,))],
        compiler_params=PARAMS,
        name="mesh_layer",
    )(meta, o, state, gains, w_own, *fetched, *fetched, other, other, *mesh, *weights)


def final_kernel(meta, counts, o, w_out, grid_in, out):
    tile = grid_in.shape[0]
    heads = jnp.concatenate([o[source(meta, k)] for k in range(MP)], axis=1)
    value = grid_in[...].astype(F32) + dot(heads, w_out[...])
    row = lax.broadcasted_iota(jnp.int32, (BLOCK, 256), 0)
    for b in range(tile // BLOCK):
        count = counts[meta[1] * 8 + pl.program_id(0) * (tile // BLOCK) + b]
        part = value[b * BLOCK : (b + 1) * BLOCK, :]
        out[b * BLOCK : (b + 1) * BLOCK, :] = jnp.where(row < count, part, 0.0).astype(BF16)


def final(meta, counts, o, w_out, grid_in):
    rows = grid_in.shape[0]
    tile = 512
    return pl.pallas_call(
        final_kernel,
        grid=(rows // tile,),
        in_specs=[
            smem(),
            smem(),
            pl.BlockSpec((MP, tile, 128), lambda i: (0, i, 0)),
            vmem(),
            pl.BlockSpec((tile, 256), lambda i: (i, 0)),
        ],
        out_specs=pl.BlockSpec((tile, 256), lambda i: (i, 0)),
        out_shape=jax.ShapeDtypeStruct((rows, 256), BF16),
        compiler_params=PARAMS,
        name="grid_final",
    )(meta, counts, o, w_out, grid_in)


def gather_heads(copies):
    return lax.all_to_all(copies, "mp", split_axis=0, concat_axis=0, tiled=True)


def program(
    grid_in, mesh_in, w_query, w_key, w_value, w_out, norm_gains,
    enc_list, proc_list, dec_list, grid_count,
):
    own_mp, own_node = lax.axis_index("mp"), lax.axis_index("nodes")
    core = own_node % 2
    meta = jnp.concatenate([
        own_mp[None].astype(jnp.int32),
        own_node[None].astype(jnp.int32),
        enc_list.reshape(-1) - (own_node - REACH) * 8,
        proc_list.reshape(-1) - (own_node - REACH) * 2,
        dec_list.reshape(-1) - (own_node - REACH) * 2,
    ])
    gains = norm_gains.reshape(6, MP, 256)
    w_query, w_key, w_value = (
        pltpu.with_memory_space_constraint(w, pltpu.HBM) for w in (w_query, w_key, w_value)
    )

    def gathered(part, name):
        pieces = [part, None, None, None]
        for k in (1, 3, 2):
            pieces[k] = swap_mp(part if name != "w" else part[k], k)
        return pieces

    def window(part):
        across = swap_chips(part, 1)
        within = swap_chips(part, 0)
        beside = swap_cores(part)
        beyond = swap_cores(jnp.where((core == 0) == (own_node // 2 % 2 == 0), within, across))
        return [across, part, within, beside, beyond]

    grid_pieces = gathered(grid_in, "g")
    grid_pieces[0] = pltpu.with_memory_space_constraint(grid_in, pltpu.HBM)

    halves = [lax.dynamic_slice_in_dim(w_out[:3], core * 512 + part * 256, 256, axis=2) for part in range(2)]
    sent = [None] * MP
    for k in (1, 2, 3):
        last = lax.dynamic_slice_in_dim(w_out[3:], (own_mp ^ k) * 256, 256, axis=2)
        sent[k] = jnp.concatenate([mesh_in.reshape(2, BLOCK, 256)] + halves + [last], axis=0)
    sent[0] = sent[1]
    arrived = gathered(sent, "w")[1:]

    kv = grid_project(1, 0, meta, grid_pieces, gains, w_key, w_value)
    grid_windows = window(kv)
    grid_q = grid_project(4, 3, meta, grid_pieces, gains, w_query)
    w_own = pltpu.with_memory_space_constraint(w_out, pltpu.HBM)
    mesh_q = mesh_start(meta, mesh_in, arrived, gains, w_query)
    o = enc_attend(meta, enc_list, grid_count, mesh_q, grid_windows)

    arrived = lax.optimization_barrier((*arrived, o))[:3]
    other = swap_cores(jnp.stack([a[2:8] for a in arrived]))
    w_last = jnp.concatenate(
        [lax.dynamic_slice_in_dim(w_out[3:], own_mp * 256, 256, axis=2)] + [a[8:] for a in arrived], axis=0
    ).reshape(512, 256)

    state = mesh_in
    for index in range(3):
        heads = gather_heads(o)
        made = layer(index, meta, heads, state, gains, w_own, arrived, other, (w_key, w_value, w_query))
        state, kv = made[0], made[1]
        near = window(kv)
        if index < 2:
            o = near_attend(PROC0, 3, meta, made[2], near)
    grid_q, w_last = lax.optimization_barrier((grid_q, w_last))
    o = near_attend(DEC0, 2, meta, grid_q, near)
    heads = gather_heads(o)
    grid_out = final(meta, grid_count, heads, w_last, grid_in)
    return grid_out, state


def solution(mesh):
    placed = (
        P("nodes", "mp"),
        P("nodes", "mp"),
        P(None, None, "mp"),
        P(None, None, "mp"),
        P(None, None, "mp"),
        P(None, "mp", None),
        P(),
        P("nodes", None),
        P("nodes", None),
        P("nodes", None),
        P(),
    )
    return jax.shard_map(
        program,
        mesh=mesh,
        in_specs=placed,
        out_specs=(P("nodes", "mp"), P("nodes", "mp")),
        check_vma=False,
    )
```

```python
import jax
import jax.numpy as jnp
from jax import lax
from jax.experimental import pallas as pl
from jax.experimental.pallas import tpu as pltpu
from jax.sharding import PartitionSpec as P


BLOCK = 128
REACH = 2
EPS = 1e-05
MP = 4
F32 = jnp.float32
BF16 = jnp.bfloat16

ENC0, PROC0, DEC0 = 2, 10, 16


PARAMS = pltpu.CompilerParams(vmem_limit_bytes=16 * 1024 * 1024)


def swap_mp(value, k):
    return lax.ppermute(value, "mp", [(s, s ^ k) for s in range(MP)])


def swap_chips(value, first):
    count = lax.axis_size("nodes") // 2
    pairs = []
    for c in range(first, count - 1, 2):
        for core in range(2):
            pairs += [(2 * c + core, 2 * c + 2 + core), (2 * c + 2 + core, 2 * c + core)]
    return lax.ppermute(value, "nodes", pairs)


def swap_cores(value):
    count = lax.axis_size("nodes")
    return lax.ppermute(value, "nodes", [(s, s ^ 1) for s in range(count)])


def smem():
    return pl.BlockSpec(memory_space=pltpu.SMEM)


def vmem():
    return pl.BlockSpec(memory_space=pltpu.VMEM)


def hbm():
    return pl.BlockSpec(memory_space=pltpu.HBM)


def copies_of(pairs, kept, sems):
    return [
        pltpu.make_async_copy(w.at[layer_index], kept.at[i], sems.at[i])
        for i, (w, layer_index) in enumerate(pairs)
    ]


def source(meta, k):
    return meta[0] ^ k


def normed(pieces):
    width = sum(p.shape[-1] for p in pieces)
    values = [p.astype(F32) for p in pieces]
    mean = sum(jnp.sum(v, axis=-1, keepdims=True) for v in values) * (1.0 / width)
    centred = [v - mean for v in values]
    spread = sum(jnp.sum(c * c, axis=-1, keepdims=True) for c in centred) * (1.0 / width)
    scale = lax.rsqrt(spread + EPS)
    return [c * scale for c in centred]


def dot(a, b):
    return jnp.dot(a, b, preferred_element_type=F32)


def grid_kernel(gain_row, count, meta, x0, x1, x2, x3, gains, *rest):
    weights, out = rest[:count], rest[count]
    rows = normed([x[...] for x in (x0, x1, x2, x3)])
    total = None
    for k in range(MP):
        src = source(meta, k)
        at = pl.ds(pl.multiple_of(src * 256, 256), 256)
        row = (rows[k] * gains[gain_row, pl.ds(src, 1), :]).astype(BF16)
        part = dot(row, jnp.concatenate([w[at, :] for w in weights], axis=1))
        total = part if total is None else total + part
    out[...] = total.astype(BF16)


def grid_project(gain_row, meta, pieces, gains, *weights):
    count = len(weights)

    def body(*refs):
        grid_kernel(gain_row, count, *refs)

    rows = pieces[0].shape[0]
    tile = 256
    return pl.pallas_call(
        body,
        grid=(rows // tile,),
        in_specs=[smem()]
        + [pl.BlockSpec((tile, 256), lambda i: (i, 0))] * MP
        + [vmem()] * (1 + count),
        out_specs=pl.BlockSpec((tile, 128 * count), lambda i: (i, 0)),
        out_shape=jax.ShapeDtypeStruct((rows, 128 * count), BF16),
        cost_estimate=pl.CostEstimate(flops=rows * 1024 * 128 * count * 2, transcendentals=0, bytes_accessed=rows * 4096),
        compiler_params=PARAMS,
        name="grid_project",
    )(meta, *pieces, gains, *weights)


def grid_query_kernel(gain_row, count, layer_index, meta, x0, x1, x2, x3, gains, *rest):
    weights, (out, kept, sems) = rest[:count], rest[count:]
    copies = copies_of([(w, layer_index) for w in weights], kept, sems)

    @pl.when(pl.program_id(0) == 0)
    def _():
        for copy in copies:
            copy.start()

    rows = normed([x[...] for x in (x0, x1, x2, x3)])

    @pl.when(pl.program_id(0) == 0)
    def _():
        for copy in copies:
            copy.wait()

    total = None
    for k in range(MP):
        src = source(meta, k)
        at = pl.ds(pl.multiple_of(src * 256, 256), 256)
        row = (rows[k] * gains[gain_row, pl.ds(src, 1), :]).astype(BF16)
        part = dot(row, jnp.concatenate([kept[i, at, :] for i in range(count)], axis=1))
        total = part if total is None else total + part
    out[...] = total.astype(BF16)


def grid_query(gain_row, layer_index, meta, pieces, gains, *weights):
    count = len(weights)

    def body(*refs):
        grid_query_kernel(gain_row, count, layer_index, *refs)

    rows = pieces[0].shape[0]
    tile = 256
    return pl.pallas_call(
        body,
        grid=(rows // tile,),
        in_specs=[smem()]
        + [pl.BlockSpec((tile, 256), lambda i: (i, 0))] * MP
        + [vmem()]
        + [hbm()] * count,
        out_specs=pl.BlockSpec((tile, 128 * count), lambda i: (i, 0)),
        out_shape=jax.ShapeDtypeStruct((rows, 128 * count), BF16),
        scratch_shapes=[pltpu.VMEM((count, 1024, 128), BF16), pltpu.SemaphoreType.DMA((count,))],
        cost_estimate=pl.CostEstimate(flops=rows * 1024 * 128 * count * 2, transcendentals=0, bytes_accessed=rows * 4096),
        compiler_params=PARAMS,
        name="grid_query",
    )(meta, *pieces, gains, *weights)


def mesh_kernel(meta, x0, a1, a2, a3, gains, w_q, q_out, kept, sems):
    copies = copies_of([(w_q, 0)], kept, sems)
    copies[0].start()
    rows = normed([x0[...]] + [a[...].reshape(2 * BLOCK, 256) for a in (a1, a2, a3)])
    copies[0].wait()
    q = None
    for k in range(MP):
        src = source(meta, k)
        at = pl.ds(pl.multiple_of(src * 256, 256), 256)
        part = dot((rows[k] * gains[0, pl.ds(src, 1), :]).astype(BF16), kept[0, at, :])
        q = part if q is None else q + part
    q_out[...] = q.astype(BF16)


def mesh_start(meta, mesh_in, arrived, gains, w_q):
    rows = mesh_in.shape[0]
    return pl.pallas_call(
        mesh_kernel,
        grid=(1,),
        in_specs=[smem(), vmem()]
        + [pl.BlockSpec((2, BLOCK, 256), lambda i: (0, 0, 0))] * 3
        + [vmem(), hbm()],
        out_specs=vmem(),
        out_shape=jax.ShapeDtypeStruct((rows, 128), BF16),
        scratch_shapes=[pltpu.VMEM((1, 1024, 128), BF16), pltpu.SemaphoreType.DMA((1,))],
        cost_estimate=pl.CostEstimate(flops=rows * 1024 * 128 * 2, transcendentals=0, bytes_accessed=rows * 4096),
        compiler_params=PARAMS,
        name="mesh_start",
    )(meta, mesh_in, *arrived, gains, w_q)


def head_rows():
    lane = lax.broadcasted_iota(jnp.int32, (1, 128), 1)
    first = jnp.where(lane < 64, 0.125, 0.0).astype(BF16)
    second = jnp.where(lane < 64, 0.0, 0.125).astype(BF16)
    return first, second


def attend_block(q, keys, values, key_ok):
    outs = []
    for row in head_rows():
        scores = lax.dot_general(
            q * row, keys, (((1,), (1,)), ((), ())), preferred_element_type=F32
        )
        if key_ok is not None:
            scores = jnp.where(key_ok, scores, -1e30)
        highest = jnp.max(scores, axis=-1, keepdims=True)
        weights = jnp.exp(scores - highest)
        total = jnp.sum(weights, axis=-1, keepdims=True)
        outs.append(dot(weights.astype(BF16), values) / total)
    lane = lax.broadcasted_iota(jnp.int32, outs[0].shape, 1)
    return jnp.where(lane < 64, outs[0], outs[1]).astype(BF16)


def window_places(meta):
    core = meta[1] % 2
    odd = meta[1] // 2 % 2
    return 4 * odd, 2, 4 - 4 * odd, 3 - 2 * core, 1 + 2 * core


def enc_kernel(meta, listed, counts, q, a0, a1, a2, a3, a4, o_out, kept):
    blocks_each = a0.shape[0] // BLOCK
    places = window_places(meta)
    for slot in range(8):
        place = meta[ENC0 + slot]
        which = place // blocks_each
        start = pl.multiple_of((place % blocks_each) * BLOCK, BLOCK)
        for w, array in zip(places, (a0, a1, a2, a3, a4)):

            @pl.when(which == w)
            def _():
                kept[slot] = array[pl.ds(start, BLOCK), :]

    lane = lax.broadcasted_iota(jnp.int32, (1, BLOCK), 1)
    for b in range(2):
        key_ok = jnp.concatenate(
            [lane < counts[listed[b, j]] for j in range(4)], axis=1
        )
        kv = kept[b * 4 : b * 4 + 4].reshape(4 * BLOCK, 256)
        o = attend_block(q[b * BLOCK : (b + 1) * BLOCK, :], kv[:, :128], kv[:, 128:], key_ok)
        for j in range(MP):
            o_out[j, b * BLOCK : (b + 1) * BLOCK, :] = o


def enc_attend(meta, listed, counts, q, windows):
    return pl.pallas_call(
        enc_kernel,
        in_specs=[smem(), smem(), smem()] + [vmem()] * 6,
        out_specs=vmem(),
        out_shape=pltpu.HBM((MP,) + q.shape, BF16),
        scratch_shapes=[pltpu.VMEM((8, BLOCK, 256), BF16)],
        compiler_params=PARAMS,
        name="enc_attend",
    )(meta, listed, counts, q, *windows)


def near_kernel(first_entry, per_block, meta, q, a0, a1, a2, a3, a4, o_out, kept):
    for w, array in zip(window_places(meta), (a0, a1, a2, a3, a4)):
        kept[2 * w] = array[0:BLOCK, :]
        kept[2 * w + 1] = array[BLOCK : 2 * BLOCK, :]
    for b in range(q.shape[0] // BLOCK):
        kv = jnp.concatenate(
            [kept[meta[first_entry + b * per_block + j]] for j in range(per_block)], axis=0
        )
        o = attend_block(q[b * BLOCK : (b + 1) * BLOCK, :], kv[:, :128], kv[:, 128:], None)
        for j in range(o_out.shape[0]):
            o_out[j, b * BLOCK : (b + 1) * BLOCK, :] = o


def near_attend(first_entry, per_block, copies, meta, q, windows):
    def body(*refs):
        near_kernel(first_entry, per_block, *refs)

    return pl.pallas_call(
        body,
        in_specs=[smem()] + [vmem()] * 6,
        out_specs=vmem(),
        out_shape=jax.ShapeDtypeStruct((copies,) + q.shape, BF16),
        scratch_shapes=[pltpu.VMEM((10, BLOCK, 256), BF16)],
        compiler_params=PARAMS,
        name="near_attend",
    )(meta, q, *windows)


def prepare_kernel(index, meta, w_own, a1, a2, a3, other, *rest):
    weights = rest[:-4]
    w_out, w_next, w_sems, sems = rest[-4:]
    core = meta[1] % 2
    copies = [
        pltpu.make_async_copy(
            w_own.at[index, :, g * 256 : (g + 1) * 256], w_out.at[g, 0:BLOCK, :], w_sems.at[g, 0]
        )
        for g in range(MP)
    ]
    for part in range(2):
        at = index + 3 * part
        for k, a in enumerate((a1, a2, a3)):
            rows = w_out.at[2 * core + part, (k + 1) * BLOCK : (k + 2) * BLOCK, :]
            copies.append(pltpu.make_async_copy(a.at[2 + at], rows, w_sems.at[part, k + 1]))
            rows = w_out.at[2 * (1 - core) + part, (k + 1) * BLOCK : (k + 2) * BLOCK, :]
            copies.append(pltpu.make_async_copy(other.at[k, at], rows, w_sems.at[2 + part, k + 1]))
    for i, w in enumerate(weights):
        copies.append(
            pltpu.make_async_copy(w.at[index + 1], w_next.at[:, i * 128 : (i + 1) * 128], sems.at[i])
        )
    for copy in copies:
        copy.start()
    for copy in copies:
        copy.wait()


def prepare(index, meta, w_own, fetched, other, weights):
    def body(*refs):
        prepare_kernel(index, *refs)

    operands = (w_own, *fetched, other, *weights)
    return pl.pallas_call(
        body,
        in_specs=[smem()] + [pl.BlockSpec(memory_space=pl.ANY)] * len(operands),
        out_specs=[vmem(), vmem()],
        out_shape=[
            jax.ShapeDtypeStruct((MP, 4 * BLOCK, 256), BF16),
            jax.ShapeDtypeStruct((1024, 128 * len(weights)), BF16),
        ],
        scratch_shapes=[pltpu.SemaphoreType.DMA((MP, MP)), pltpu.SemaphoreType.DMA((3,))],
        compiler_params=PARAMS,
        name="layer_weights",
    )(meta, *operands)


def finish_layer(gain_row, gains, new, w_next):
    rows = normed([new[g] for g in range(MP)])
    row = jnp.concatenate(
        [(rows[g] * gains[gain_row, g : g + 1, :]).astype(BF16) for g in range(MP)], axis=1
    )
    return dot(row, w_next()).astype(BF16)


def first_layer_kernel(meta, o, state, gains, w_own, a1, a2, a3, other, w_k, w_v, w_q, *rest):
    new, kv_out, q_out, kept, sems = rest
    copies = copies_of([(w_k, 1), (w_v, 1), (w_q, 1)], kept, sems)
    for copy in copies:
        copy.start()
    heads = jnp.concatenate([o[source(meta, k)] for k in range(MP)], axis=1)
    new[meta[0]] = state[...]
    for k, a in enumerate((a1, a2, a3)):
        new[source(meta, k + 1)] = a[0:2].reshape(2 * BLOCK, 256)
    core = meta[1] % 2
    for part in range(4):
        at = 3 * (part % 2)
        if part < 2:
            g = 2 * core + part
            fetched = [a[2 + at] for a in (a1, a2, a3)]
        else:
            g = 2 * (1 - core) + part - 2
            fetched = [other[k, at] for k in range(MP - 1)]
        own = w_own[0, :, pl.ds(pl.multiple_of(g * 256, 256), 256)]
        new[g] = (new[g].astype(F32) + dot(heads, jnp.concatenate([own] + fetched, axis=0))).astype(BF16)

    def w_next():
        for copy in copies:
            copy.wait()
        return jnp.concatenate([kept[i] for i in range(3)], axis=1)

    result = finish_layer(2, gains, new, w_next)
    kv_out[...] = result[:, :256]
    q_out[...] = result[:, 256:]


def first_layer(meta, o, state, gains, w_own, fetched, other, weights):
    rows = o.shape[1]
    return pl.pallas_call(
        first_layer_kernel,
        in_specs=[smem()] + [vmem()] * 8 + [hbm()] * 3,
        out_specs=[vmem()] * 3,
        out_shape=[
            jax.ShapeDtypeStruct((MP, rows, 256), BF16),
            jax.ShapeDtypeStruct((rows, 256), BF16),
            jax.ShapeDtypeStruct((rows, 128), BF16),
        ],
        scratch_shapes=[pltpu.VMEM((3, 1024, 128), BF16), pltpu.SemaphoreType.DMA((3,))],
        compiler_params=PARAMS,
        name="first_layer",
    )(meta, o, state, gains, w_own, *fetched, other, *weights)


def layer_kernel(gain_row, o, state, gains, w_out, w_next, *rest):
    last = gain_row == 5
    state_out, kv_out, new = rest[0], rest[1], rest[-1]
    own = lax.axis_index("mp")
    heads = jnp.concatenate([o[own ^ k] for k in range(MP)], axis=1)
    for g in range(MP):
        new[g] = (state[g].astype(F32) + dot(heads, w_out[g])).astype(BF16)
        if not last:
            state_out[g] = new[g]
    if last:
        state_out[...] = new[own]
    result = finish_layer(gain_row, gains, new, lambda: w_next[...])
    kv_out[...] = result[:, :256]
    if not last:
        rest[2][...] = result[:, 256:]


def layer(gain_row, o, state, gains, prepared):
    def body(*refs):
        layer_kernel(gain_row, *refs)

    last = gain_row == 5
    rows = o.shape[1]
    shapes = [
        jax.ShapeDtypeStruct((rows, 256) if last else (MP, rows, 256), BF16),
        jax.ShapeDtypeStruct((rows, 256), BF16),
    ]
    if not last:
        shapes.append(jax.ShapeDtypeStruct((rows, 128), BF16))
    return pl.pallas_call(
        body,
        in_specs=[vmem()] * 5,
        out_specs=[vmem()] * len(shapes),
        out_shape=shapes,
        scratch_shapes=[pltpu.VMEM((MP, rows, 256), BF16)],
        compiler_params=PARAMS,
        name="mesh_layer",
    )(o, state, gains, *prepared)


def final_kernel(meta, counts, o0, o1, o2, o3, w_out, grid_in, out):
    tile = grid_in.shape[0]
    heads = jnp.concatenate([o[...] for o in (o0, o1, o2, o3)], axis=1)
    value = grid_in[...].astype(F32) + dot(heads, w_out[...])
    row = lax.broadcasted_iota(jnp.int32, (BLOCK, 256), 0)
    for b in range(tile // BLOCK):
        count = counts[meta[1] * 8 + pl.program_id(0) * (tile // BLOCK) + b]
        part = value[b * BLOCK : (b + 1) * BLOCK, :]
        out[b * BLOCK : (b + 1) * BLOCK, :] = jnp.where(row < count, part, 0.0).astype(BF16)


def final(meta, counts, o, w_out, grid_in):
    rows = grid_in.shape[0]
    tile = 512
    return pl.pallas_call(
        final_kernel,
        grid=(rows // tile,),
        in_specs=[
            smem(),
            smem(),
        ]
        + [pl.BlockSpec((tile, 128), lambda i: (i, 0))] * MP
        + [
            vmem(),
            pl.BlockSpec((tile, 256), lambda i: (i, 0)),
        ],
        out_specs=pl.BlockSpec((tile, 256), lambda i: (i, 0)),
        out_shape=jax.ShapeDtypeStruct((rows, 256), BF16),
        compiler_params=PARAMS,
        name="grid_final",
    )(meta, counts, *o, w_out, grid_in)


def gather_heads(copies):
    return lax.all_to_all(copies, "mp", split_axis=0, concat_axis=0, tiled=True)


def program(
    grid_in, mesh_in, w_query, w_key, w_value, w_out, norm_gains,
    enc_list, proc_list, dec_list, grid_count,
):
    own_mp, own_node = lax.axis_index("mp"), lax.axis_index("nodes")
    core = own_node % 2
    meta = jnp.concatenate([
        own_mp[None].astype(jnp.int32),
        own_node[None].astype(jnp.int32),
        enc_list.reshape(-1) - (own_node - REACH) * 8,
        proc_list.reshape(-1) - (own_node - REACH) * 2,
        dec_list.reshape(-1) - (own_node - REACH) * 2,
    ])
    gains = norm_gains.reshape(6, MP, 256)
    w_first = (w_key[0], w_value[0])
    w_query, w_key, w_value = (
        pltpu.with_memory_space_constraint(w, pltpu.HBM) for w in (w_query, w_key, w_value)
    )

    def gathered(part, name):
        pieces = [part, None, None, None]
        for k in (1, 3, 2):
            pieces[k] = swap_mp(part if name != "w" else part[k], k)
        return pieces

    def window(part):
        across = swap_chips(part, 1)
        within = swap_chips(part, 0)
        beside = swap_cores(part)
        beyond = swap_cores(jnp.where((core == 0) == (own_node // 2 % 2 == 0), within, across))
        return [across, part, within, beside, beyond]

    grid_pieces = gathered(grid_in, "g")
    grid_pieces[0] = pltpu.with_memory_space_constraint(grid_in, pltpu.HBM)

    halves = [lax.dynamic_slice_in_dim(w_out[:3], core * 512 + part * 256, 256, axis=2) for part in range(2)]
    sent = [None] * MP
    for k in (1, 2, 3):
        last = lax.dynamic_slice_in_dim(w_out[3:], (own_mp ^ k) * 256, 256, axis=2)
        sent[k] = jnp.concatenate([mesh_in.reshape(2, BLOCK, 256)] + halves + [last], axis=0)
    sent[0] = sent[1]
    arrived = gathered(sent, "w")[1:]

    kv = grid_project(1, meta, grid_pieces, gains, *w_first)
    grid_windows = window(kv)
    grid_q = grid_query(4, 3, meta, grid_pieces, gains, w_query)
    w_own = pltpu.with_memory_space_constraint(w_out, pltpu.HBM)
    mesh_q = mesh_start(meta, mesh_in, arrived, gains, w_query)
    o = enc_attend(meta, enc_list, grid_count, mesh_q, grid_windows)

    arrived = lax.optimization_barrier((*arrived, o))[:3]
    other = swap_cores(jnp.stack([a[2:8] for a in arrived]))
    w_last = jnp.concatenate(
        [lax.dynamic_slice_in_dim(w_out[3:], own_mp * 256, 256, axis=2)] + [a[8:] for a in arrived], axis=0
    ).reshape(512, 256)

    state = mesh_in
    for index in range(3):
        heads = gather_heads(o)
        if index == 0:
            made = first_layer(meta, heads, state, gains, w_out, arrived, other, (w_key, w_value, w_query))
        else:
            made = layer(3 if index == 1 else 5, heads, state, gains, prepared)
        state, kv = made[0], made[1]
        near = window(kv)
        if index < 2:
            weights = (w_key, w_value, w_query) if index == 0 else (w_key, w_value)
            prepared = prepare(index + 1, meta, w_own, arrived, other, weights)
            o = near_attend(PROC0, 3, MP, meta, made[2], near)
    grid_q, w_last = lax.optimization_barrier((grid_q, w_last))
    o = near_attend(DEC0, 2, 1, meta, grid_q, near)
    heads = gathered(o[0], "d")
    grid_out = final(meta, grid_count, heads, w_last, grid_in)
    return grid_out, state


def solution(mesh):
    placed = (
        P("nodes", "mp"),
        P("nodes", "mp"),
        P(None, None, "mp"),
        P(None, None, "mp"),
        P(None, None, "mp"),
        P(None, "mp", None),
        P(),
        P("nodes", None),
        P("nodes", None),
        P("nodes", None),
        P(),
    )
    return jax.shard_map(
        program,
        mesh=mesh,
        in_specs=placed,
        out_specs=(P("nodes", "mp"), P("nodes", "mp")),
        check_vma=False,
    )
```

```python
import jax
import jax.numpy as jnp
from jax import lax
from jax.experimental import pallas as pl
from jax.experimental.pallas import tpu as pltpu
from jax.sharding import PartitionSpec as P


BLOCK = 128
REACH = 2
EPS = 1e-05
MP = 4
F32 = jnp.float32
BF16 = jnp.bfloat16

ENC0, PROC0, DEC0 = 2, 10, 16


PARAMS = pltpu.CompilerParams(vmem_limit_bytes=16 * 1024 * 1024)


def swap_mp(value, k):
    return lax.ppermute(value, "mp", [(s, s ^ k) for s in range(MP)])


def swap_chips(value, first):
    count = lax.axis_size("nodes") // 2
    pairs = []
    for c in range(first, count - 1, 2):
        for core in range(2):
            pairs += [(2 * c + core, 2 * c + 2 + core), (2 * c + 2 + core, 2 * c + core)]
    return lax.ppermute(value, "nodes", pairs)


def swap_cores(value):
    count = lax.axis_size("nodes")
    return lax.ppermute(value, "nodes", [(s, s ^ 1) for s in range(count)])


def smem():
    return pl.BlockSpec(memory_space=pltpu.SMEM)


def vmem():
    return pl.BlockSpec(memory_space=pltpu.VMEM)


def hbm():
    return pl.BlockSpec(memory_space=pltpu.HBM)


def copies_of(pairs, kept, sems):
    return [
        pltpu.make_async_copy(w.at[layer_index], kept.at[i], sems.at[i])
        for i, (w, layer_index) in enumerate(pairs)
    ]


def source(meta, k):
    return meta[0] ^ k


def normed(pieces):
    width = sum(p.shape[-1] for p in pieces)
    values = [p.astype(F32) for p in pieces]
    mean = sum(jnp.sum(v, axis=-1, keepdims=True) for v in values) * (1.0 / width)
    centred = [v - mean for v in values]
    spread = sum(jnp.sum(c * c, axis=-1, keepdims=True) for c in centred) * (1.0 / width)
    scale = lax.rsqrt(spread + EPS)
    return [c * scale for c in centred]


def dot(a, b):
    return jnp.dot(a, b, preferred_element_type=F32)


def grid_kernel(gain_row, count, meta, x0, x1, x2, x3, gains, *rest):
    weights, out = rest[:count], rest[count]
    rows = normed([x[...] for x in (x0, x1, x2, x3)])
    total = None
    for k in range(MP):
        src = source(meta, k)
        at = pl.ds(pl.multiple_of(src * 256, 256), 256)
        row = (rows[k] * gains[gain_row, pl.ds(src, 1), :]).astype(BF16)
        part = dot(row, jnp.concatenate([w[at, :] for w in weights], axis=1))
        total = part if total is None else total + part
    out[...] = total.astype(BF16)


def grid_project(gain_row, meta, pieces, gains, *weights):
    count = len(weights)

    def body(*refs):
        grid_kernel(gain_row, count, *refs)

    rows = pieces[0].shape[0]
    tile = 256
    return pl.pallas_call(
        body,
        grid=(rows // tile,),
        in_specs=[smem()]
        + [pl.BlockSpec((tile, 256), lambda i: (i, 0))] * MP
        + [vmem()] * (1 + count),
        out_specs=pl.BlockSpec((tile, 128 * count), lambda i: (i, 0)),
        out_shape=jax.ShapeDtypeStruct((rows, 128 * count), BF16),
        cost_estimate=pl.CostEstimate(flops=rows * 1024 * 128 * count * 2, transcendentals=0, bytes_accessed=rows * 4096),
        compiler_params=PARAMS,
        name="grid_project",
    )(meta, *pieces, gains, *weights)


def grid_query_kernel(gain_row, count, layer_index, meta, x0, x1, x2, x3, gains, *rest):
    weights, (out, kept, sems) = rest[:count], rest[count:]
    copies = copies_of([(w, layer_index) for w in weights], kept, sems)

    @pl.when(pl.program_id(0) == 0)
    def _():
        for copy in copies:
            copy.start()

    rows = normed([x[...] for x in (x0, x1, x2, x3)])

    @pl.when(pl.program_id(0) == 0)
    def _():
        for copy in copies:
            copy.wait()

    total = None
    for k in range(MP):
        src = source(meta, k)
        at = pl.ds(pl.multiple_of(src * 256, 256), 256)
        row = (rows[k] * gains[gain_row, pl.ds(src, 1), :]).astype(BF16)
        part = dot(row, jnp.concatenate([kept[i, at, :] for i in range(count)], axis=1))
        total = part if total is None else total + part
    out[...] = total.astype(BF16)


def grid_query(gain_row, layer_index, meta, pieces, gains, *weights):
    count = len(weights)

    def body(*refs):
        grid_query_kernel(gain_row, count, layer_index, *refs)

    rows = pieces[0].shape[0]
    tile = 256
    return pl.pallas_call(
        body,
        grid=(rows // tile,),
        in_specs=[smem()]
        + [pl.BlockSpec((tile, 256), lambda i: (i, 0))] * MP
        + [vmem()]
        + [hbm()] * count,
        out_specs=pl.BlockSpec((tile, 128 * count), lambda i: (i, 0)),
        out_shape=jax.ShapeDtypeStruct((rows, 128 * count), BF16),
        scratch_shapes=[pltpu.VMEM((count, 1024, 128), BF16), pltpu.SemaphoreType.DMA((count,))],
        cost_estimate=pl.CostEstimate(flops=rows * 1024 * 128 * count * 2, transcendentals=0, bytes_accessed=rows * 4096),
        compiler_params=PARAMS,
        name="grid_query",
    )(meta, *pieces, gains, *weights)


def mesh_kernel(meta, x0, a1, a2, a3, gains, w_q, q_out, kept, sems):
    copies = copies_of([(w_q, 0)], kept, sems)
    copies[0].start()
    rows = normed([x0[...]] + [a[...].reshape(2 * BLOCK, 256) for a in (a1, a2, a3)])
    copies[0].wait()
    q = None
    for k in range(MP):
        src = source(meta, k)
        at = pl.ds(pl.multiple_of(src * 256, 256), 256)
        part = dot((rows[k] * gains[0, pl.ds(src, 1), :]).astype(BF16), kept[0, at, :])
        q = part if q is None else q + part
    q_out[...] = q.astype(BF16)


def mesh_start(meta, mesh_in, arrived, gains, w_q):
    rows = mesh_in.shape[0]
    return pl.pallas_call(
        mesh_kernel,
        grid=(1,),
        in_specs=[smem(), vmem()]
        + [pl.BlockSpec((2, BLOCK, 256), lambda i: (0, 0, 0))] * 3
        + [vmem(), hbm()],
        out_specs=vmem(),
        out_shape=jax.ShapeDtypeStruct((rows, 128), BF16),
        scratch_shapes=[pltpu.VMEM((1, 1024, 128), BF16), pltpu.SemaphoreType.DMA((1,))],
        cost_estimate=pl.CostEstimate(flops=rows * 1024 * 128 * 2, transcendentals=0, bytes_accessed=rows * 4096),
        compiler_params=PARAMS,
        name="mesh_start",
    )(meta, mesh_in, *arrived, gains, w_q)


def head_rows():
    lane = lax.broadcasted_iota(jnp.int32, (1, 128), 1)
    first = jnp.where(lane < 64, 0.125, 0.0).astype(BF16)
    second = jnp.where(lane < 64, 0.0, 0.125).astype(BF16)
    return first, second


def attend_block(q, keys, values, key_ok):
    outs = []
    for row in head_rows():
        scores = lax.dot_general(
            q * row, keys, (((1,), (1,)), ((), ())), preferred_element_type=F32
        )
        if key_ok is not None:
            scores = jnp.where(key_ok, scores, -1e30)
        highest = jnp.max(scores, axis=-1, keepdims=True)
        weights = jnp.exp(scores - highest)
        total = jnp.sum(weights, axis=-1, keepdims=True)
        outs.append(dot(weights.astype(BF16), values) / total)
    lane = lax.broadcasted_iota(jnp.int32, outs[0].shape, 1)
    return jnp.where(lane < 64, outs[0], outs[1]).astype(BF16)


def window_places(meta):
    core = meta[1] % 2
    odd = meta[1] // 2 % 2
    return 4 * odd, 2, 4 - 4 * odd, 3 - 2 * core, 1 + 2 * core


def enc_kernel(meta, listed, counts, q, a0, a1, a2, a3, a4, o_out, kept):
    blocks_each = a0.shape[0] // BLOCK
    places = window_places(meta)
    for slot in range(8):
        place = meta[ENC0 + slot]
        which = place // blocks_each
        start = pl.multiple_of((place % blocks_each) * BLOCK, BLOCK)
        for w, array in zip(places, (a0, a1, a2, a3, a4)):

            @pl.when(which == w)
            def _():
                kept[slot] = array[pl.ds(start, BLOCK), :]

    lane = lax.broadcasted_iota(jnp.int32, (1, BLOCK), 1)
    for b in range(2):
        key_ok = jnp.concatenate(
            [lane < counts[listed[b, j]] for j in range(4)], axis=1
        )
        kv = kept[b * 4 : b * 4 + 4].reshape(4 * BLOCK, 256)
        o = attend_block(q[b * BLOCK : (b + 1) * BLOCK, :], kv[:, :128], kv[:, 128:], key_ok)
        for j in range(MP):
            o_out[j, b * BLOCK : (b + 1) * BLOCK, :] = o


def enc_attend(meta, listed, counts, q, windows):
    return pl.pallas_call(
        enc_kernel,
        in_specs=[smem(), smem(), smem()] + [vmem()] * 6,
        out_specs=vmem(),
        out_shape=pltpu.HBM((MP,) + q.shape, BF16),
        scratch_shapes=[pltpu.VMEM((8, BLOCK, 256), BF16)],
        compiler_params=PARAMS,
        name="enc_attend",
    )(meta, listed, counts, q, *windows)


def near_kernel(first_entry, per_block, meta, q, a0, a1, a2, a3, a4, o_out, kept):
    for w, array in zip(window_places(meta), (a0, a1, a2, a3, a4)):
        kept[2 * w] = array[0:BLOCK, :]
        kept[2 * w + 1] = array[BLOCK : 2 * BLOCK, :]
    for b in range(q.shape[0] // BLOCK):
        kv = jnp.concatenate(
            [kept[meta[first_entry + b * per_block + j]] for j in range(per_block)], axis=0
        )
        o = attend_block(q[b * BLOCK : (b + 1) * BLOCK, :], kv[:, :128], kv[:, 128:], None)
        for j in range(MP):
            o_out[j, b * BLOCK : (b + 1) * BLOCK, :] = o


def near_attend(first_entry, per_block, meta, q, windows):
    def body(*refs):
        near_kernel(first_entry, per_block, *refs)

    return pl.pallas_call(
        body,
        in_specs=[smem()] + [vmem()] * 6,
        out_specs=vmem(),
        out_shape=jax.ShapeDtypeStruct((MP,) + q.shape, BF16),
        scratch_shapes=[pltpu.VMEM((10, BLOCK, 256), BF16)],
        compiler_params=PARAMS,
        name="near_attend",
    )(meta, q, *windows)


def prepare_kernel(index, meta, w_own, a1, a2, a3, other, *rest):
    weights = rest[:-4]
    w_out, w_next, w_sems, sems = rest[-4:]
    core = meta[1] % 2
    copies = [
        pltpu.make_async_copy(
            w_own.at[index, :, g * 256 : (g + 1) * 256], w_out.at[g, 0:BLOCK, :], w_sems.at[g, 0]
        )
        for g in range(MP)
    ]
    for part in range(2):
        at = index + 3 * part
        for k, a in enumerate((a1, a2, a3)):
            rows = w_out.at[2 * core + part, (k + 1) * BLOCK : (k + 2) * BLOCK, :]
            copies.append(pltpu.make_async_copy(a.at[2 + at], rows, w_sems.at[part, k + 1]))
            rows = w_out.at[2 * (1 - core) + part, (k + 1) * BLOCK : (k + 2) * BLOCK, :]
            copies.append(pltpu.make_async_copy(other.at[k, at], rows, w_sems.at[2 + part, k + 1]))
    for i, w in enumerate(weights):
        copies.append(
            pltpu.make_async_copy(w.at[index + 1], w_next.at[:, i * 128 : (i + 1) * 128], sems.at[i])
        )
    for copy in copies:
        copy.start()
    for copy in copies:
        copy.wait()


def prepare(index, meta, w_own, fetched, other, weights):
    def body(*refs):
        prepare_kernel(index, *refs)

    operands = (w_own, *fetched, other, *weights)
    return pl.pallas_call(
        body,
        in_specs=[smem()] + [pl.BlockSpec(memory_space=pl.ANY)] * len(operands),
        out_specs=[vmem(), vmem()],
        out_shape=[
            jax.ShapeDtypeStruct((MP, 4 * BLOCK, 256), BF16),
            jax.ShapeDtypeStruct((1024, 128 * len(weights)), BF16),
        ],
        scratch_shapes=[pltpu.SemaphoreType.DMA((MP, MP)), pltpu.SemaphoreType.DMA((3,))],
        compiler_params=PARAMS,
        name="layer_weights",
    )(meta, *operands)


def finish_layer(gain_row, gains, new, w_next):
    rows = normed([new[g] for g in range(MP)])
    row = jnp.concatenate(
        [(rows[g] * gains[gain_row, g : g + 1, :]).astype(BF16) for g in range(MP)], axis=1
    )
    return dot(row, w_next()).astype(BF16)


def first_layer_kernel(meta, o, state, gains, w_own, a1, a2, a3, other, w_k, w_v, w_q, *rest):
    new, kv_out, q_out, kept, sems = rest
    copies = copies_of([(w_k, 1), (w_v, 1), (w_q, 1)], kept, sems)
    for copy in copies:
        copy.start()
    heads = jnp.concatenate([o[source(meta, k)] for k in range(MP)], axis=1)
    new[meta[0]] = state[...]
    for k, a in enumerate((a1, a2, a3)):
        new[source(meta, k + 1)] = a[0:2].reshape(2 * BLOCK, 256)
    core = meta[1] % 2
    for part in range(4):
        at = 3 * (part % 2)
        if part < 2:
            g = 2 * core + part
            fetched = [a[2 + at] for a in (a1, a2, a3)]
        else:
            g = 2 * (1 - core) + part - 2
            fetched = [other[k, at] for k in range(MP - 1)]
        own = w_own[0, :, pl.ds(pl.multiple_of(g * 256, 256), 256)]
        new[g] = (new[g].astype(F32) + dot(heads, jnp.concatenate([own] + fetched, axis=0))).astype(BF16)

    def w_next():
        for copy in copies:
            copy.wait()
        return jnp.concatenate([kept[i] for i in range(3)], axis=1)

    result = finish_layer(2, gains, new, w_next)
    kv_out[...] = result[:, :256]
    q_out[...] = result[:, 256:]


def first_layer(meta, o, state, gains, w_own, fetched, other, weights):
    rows = o.shape[1]
    return pl.pallas_call(
        first_layer_kernel,
        in_specs=[smem()] + [vmem()] * 8 + [hbm()] * 3,
        out_specs=[vmem()] * 3,
        out_shape=[
            jax.ShapeDtypeStruct((MP, rows, 256), BF16),
            jax.ShapeDtypeStruct((rows, 256), BF16),
            jax.ShapeDtypeStruct((rows, 128), BF16),
        ],
        scratch_shapes=[pltpu.VMEM((3, 1024, 128), BF16), pltpu.SemaphoreType.DMA((3,))],
        compiler_params=PARAMS,
        name="first_layer",
    )(meta, o, state, gains, w_own, *fetched, other, *weights)


def layer_kernel(gain_row, o, state, gains, w_out, w_next, *rest):
    last = gain_row == 5
    state_out, kv_out, new = rest[0], rest[1], rest[-1]
    own = lax.axis_index("mp")
    heads = jnp.concatenate([o[own ^ k] for k in range(MP)], axis=1)
    for g in range(MP):
        new[g] = (state[g].astype(F32) + dot(heads, w_out[g])).astype(BF16)
        if not last:
            state_out[g] = new[g]
    if last:
        state_out[...] = new[own]
    result = finish_layer(gain_row, gains, new, lambda: w_next[...])
    kv_out[...] = result[:, :256]
    if not last:
        rest[2][...] = result[:, 256:]


def layer(gain_row, o, state, gains, prepared):
    def body(*refs):
        layer_kernel(gain_row, *refs)

    last = gain_row == 5
    rows = o.shape[1]
    shapes = [
        jax.ShapeDtypeStruct((rows, 256) if last else (MP, rows, 256), BF16),
        jax.ShapeDtypeStruct((rows, 256), BF16),
    ]
    if not last:
        shapes.append(jax.ShapeDtypeStruct((rows, 128), BF16))
    return pl.pallas_call(
        body,
        in_specs=[vmem()] * 5,
        out_specs=[vmem()] * len(shapes),
        out_shape=shapes,
        scratch_shapes=[pltpu.VMEM((MP, rows, 256), BF16)],
        compiler_params=PARAMS,
        name="mesh_layer",
    )(o, state, gains, *prepared)


def final_kernel(meta, counts, o, w_out, grid_in, out):
    tile = grid_in.shape[0]
    heads = jnp.concatenate([o[source(meta, k)] for k in range(MP)], axis=1)
    value = grid_in[...].astype(F32) + dot(heads, w_out[...])
    row = lax.broadcasted_iota(jnp.int32, (BLOCK, 256), 0)
    for b in range(tile // BLOCK):
        count = counts[meta[1] * 8 + pl.program_id(0) * (tile // BLOCK) + b]
        part = value[b * BLOCK : (b + 1) * BLOCK, :]
        out[b * BLOCK : (b + 1) * BLOCK, :] = jnp.where(row < count, part, 0.0).astype(BF16)


def final(meta, counts, o, w_out, grid_in):
    rows = grid_in.shape[0]
    tile = 512
    return pl.pallas_call(
        final_kernel,
        grid=(rows // tile,),
        in_specs=[
            smem(),
            smem(),
            pl.BlockSpec((MP, tile, 128), lambda i: (0, i, 0)),
            vmem(),
            pl.BlockSpec((tile, 256), lambda i: (i, 0)),
        ],
        out_specs=pl.BlockSpec((tile, 256), lambda i: (i, 0)),
        out_shape=jax.ShapeDtypeStruct((rows, 256), BF16),
        compiler_params=PARAMS,
        name="grid_final",
    )(meta, counts, o, w_out, grid_in)


def gather_heads(copies):
    return lax.all_to_all(copies, "mp", split_axis=0, concat_axis=0, tiled=True)


def program(
    grid_in, mesh_in, w_query, w_key, w_value, w_out, norm_gains,
    enc_list, proc_list, dec_list, grid_count,
):
    own_mp, own_node = lax.axis_index("mp"), lax.axis_index("nodes")
    core = own_node % 2
    meta = jnp.concatenate([
        own_mp[None].astype(jnp.int32),
        own_node[None].astype(jnp.int32),
        enc_list.reshape(-1) - (own_node - REACH) * 8,
        proc_list.reshape(-1) - (own_node - REACH) * 2,
        dec_list.reshape(-1) - (own_node - REACH) * 2,
    ])
    gains = norm_gains.reshape(6, MP, 256)
    w_first = (w_key[0], w_value[0])
    w_query, w_key, w_value = (
        pltpu.with_memory_space_constraint(w, pltpu.HBM) for w in (w_query, w_key, w_value)
    )

    def gathered(part, name):
        pieces = [part, None, None, None]
        for k in (1, 3, 2):
            pieces[k] = swap_mp(part if name != "w" else part[k], k)
        return pieces

    def window(part):
        across = swap_chips(part, 1)
        within = swap_chips(part, 0)
        beside = swap_cores(part)
        beyond = swap_cores(jnp.where((core == 0) == (own_node // 2 % 2 == 0), within, across))
        return [across, part, within, beside, beyond]

    grid_pieces = gathered(grid_in, "g")
    grid_pieces[0] = pltpu.with_memory_space_constraint(grid_in, pltpu.HBM)

    halves = [lax.dynamic_slice_in_dim(w_out[:3], core * 512 + part * 256, 256, axis=2) for part in range(2)]
    sent = [None] * MP
    for k in (1, 2, 3):
        last = lax.dynamic_slice_in_dim(w_out[3:], (own_mp ^ k) * 256, 256, axis=2)
        sent[k] = jnp.concatenate([mesh_in.reshape(2, BLOCK, 256)] + halves + [last], axis=0)
    sent[0] = sent[1]
    arrived = gathered(sent, "w")[1:]

    kv = grid_project(1, meta, grid_pieces, gains, *w_first)
    grid_windows = window(kv)
    grid_q = grid_query(4, 3, meta, grid_pieces, gains, w_query)
    w_own = pltpu.with_memory_space_constraint(w_out, pltpu.HBM)
    mesh_q = mesh_start(meta, mesh_in, arrived, gains, w_query)
    o = enc_attend(meta, enc_list, grid_count, mesh_q, grid_windows)

    arrived = lax.optimization_barrier((*arrived, o))[:3]
    other = swap_cores(jnp.stack([a[2:8] for a in arrived]))
    w_last = jnp.concatenate(
        [lax.dynamic_slice_in_dim(w_out[3:], own_mp * 256, 256, axis=2)] + [a[8:] for a in arrived], axis=0
    ).reshape(512, 256)

    state = mesh_in
    for index in range(3):
        heads = gather_heads(o)
        if index == 0:
            made = first_layer(meta, heads, state, gains, w_out, arrived, other, (w_key, w_value, w_query))
        else:
            made = layer(3 if index == 1 else 5, heads, state, gains, prepared)
        state, kv = made[0], made[1]
        near = window(kv)
        if index < 2:
            weights = (w_key, w_value, w_query) if index == 0 else (w_key, w_value)
            prepared = prepare(index + 1, meta, w_own, arrived, other, weights)
            o = near_attend(PROC0, 3, meta, made[2], near)
    grid_q, w_last = lax.optimization_barrier((grid_q, w_last))
    o = near_attend(DEC0, 2, meta, grid_q, near)
    heads = gather_heads(o)
    grid_out = final(meta, grid_count, heads, w_last, grid_in)
    return grid_out, state


def solution(mesh):
    placed = (
        P("nodes", "mp"),
        P("nodes", "mp"),
        P(None, None, "mp"),
        P(None, None, "mp"),
        P(None, None, "mp"),
        P(None, "mp", None),
        P(),
        P("nodes", None),
        P("nodes", None),
        P("nodes", None),
        P(),
    )
    return jax.shard_map(
        program,
        mesh=mesh,
        in_specs=placed,
        out_specs=(P("nodes", "mp"), P("nodes", "mp")),
        check_vma=False,
    )
```
